32 devices in a mesh: dp: 4 (over y, z), sp: 8 (over x, core).
Axes of the slice: x: 4, y: 2, z: 2, core: 2. Of those that a mesh axis runs over, the one named last changes fastest.
The devices are a block of a 4x4x8 slice.
Arguments:
- hidden: bfloat16 [512, 4096], P('dp'), parts along dimension 0
- w_norm: bfloat16 [4096], replicated
- w_q: bfloat16 [4096, 4096], replicated
- w_k: bfloat16 [4096, 256], replicated
- w_v: bfloat16 [4096, 256], replicated
- w_o: bfloat16 [4096, 4096], replicated
- k_cache: bfloat16 [512, 1024, 256], P('dp', 'sp'), parts along dimension 0
- v_cache: bfloat16 [512, 1024, 256], P('dp', 'sp'), parts along dimension 0
- cache_len: int32 [512], P('dp'), parts along dimension 0
Outputs:
- output 1: bfloat16 [512, 4096], P('dp'), parts along dimension 0
- output 2: bfloat16 [512, 1024, 256], P('dp', 'sp'), parts along dimension 0
- output 3: bfloat16 [512, 1024, 256], P('dp', 'sp'), parts along dimension 0
There are 4 independent parts. The reference program is written for one: setup_inputs(seed, part) draws one part's arguments, and reference() takes and returns one part's arrays. A program takes and returns all parts, laid end to end along the dimension named above; an argument that names none is the same for every part.
All inputs are finite; a program needn't handle non-finite values.
Results may differ from the reference program's by a relative error of at most 0.0135738.
Values sent between devices are 32-bit elements.
A program may use at most 768 MiB of HBM per device.

```python
import math
import jax
import jax.numpy as jnp
from jax import lax

D = 4096
HEADS = 16
HEAD = 256
ROWS = 128
SEQ = 1024

ROPE_BASE = 10000.0
EPSILON = 1e-6


def rotate_half(vectors, cos_t, sin_t):
    half_dim = vectors.shape[-1] // 2
    lower_half = vectors[..., :half_dim]
    upper_half = vectors[..., half_dim:]
    return jnp.concatenate([lower_half * cos_t - upper_half * sin_t, upper_half * cos_t + lower_half * sin_t], axis=-1)


def setup_inputs(seed: int = 0, part: int = 0) -> dict:
    base_key = jax.random.key(seed)
    shared_keys = jax.random.split(base_key, 5)
    part_keys = jax.random.split(jax.random.fold_in(base_key, part), 5)
    width = HEADS * HEAD
    score_spread = math.sqrt(max(math.log(SEQ / 16.0), 1.0))
    align = (1.5 * math.log(SEQ) - 3.5) * HEADS / math.sqrt(HEAD)
    hidden = jax.random.normal(part_keys[0], (ROWS, D), jnp.float32)
    w_norm = 0.5 * jax.random.normal(shared_keys[0], (D,), jnp.float32)
    w_q = jax.random.normal(shared_keys[1], (D, width), jnp.float32) * D ** -0.5
    q_mean = w_q.reshape(D, HEADS, HEAD).mean(axis=1)
    w_k = align * q_mean + jax.random.normal(shared_keys[2], (D, HEAD), jnp.float32) * D ** -0.5
    w_v = jax.random.normal(shared_keys[3], (D, HEAD), jnp.float32) * D ** -0.5
    w_o = jax.random.normal(shared_keys[4], (width, D), jnp.float32) * (3.0 * width ** -0.5)
    key_scale = score_spread * jax.random.uniform(part_keys[1], (ROWS, SEQ, 1), jnp.float32, minval=0.5, maxval=1.5)
    k_cache = jax.random.normal(part_keys[2], (ROWS, SEQ, HEAD), jnp.float32) * key_scale
    v_cache = jax.random.normal(part_keys[3], (ROWS, SEQ, HEAD), jnp.float32)
    row_ids = jnp.arange(ROWS)
    lengths = jax.random.randint(part_keys[4], (ROWS,), SEQ // 8, SEQ)
    lengths = jnp.where(row_ids == 0, SEQ - 1, jnp.where(row_ids == ROWS - 1, SEQ // 8, lengths))
    return {'hidden': hidden.astype(jnp.bfloat16), 'w_norm': w_norm.astype(jnp.bfloat16), 'w_q': w_q.astype(jnp.bfloat16), 'w_k': w_k.astype(jnp.bfloat16), 'w_v': w_v.astype(jnp.bfloat16), 'w_o': w_o.astype(jnp.bfloat16), 'k_cache': k_cache.astype(jnp.bfloat16), 'v_cache': v_cache.astype(jnp.bfloat16), 'cache_len': lengths.astype(jnp.int32)}


def reference(hidden, w_norm, w_q, w_k, w_v, w_o, k_cache, v_cache, cache_len):
    x_f32 = hidden.astype(jnp.float32)
    inv_rms = lax.rsqrt(jnp.mean(x_f32 * x_f32, axis=-1, keepdims=True) + EPSILON)
    x_norm = (x_f32 * inv_rms * (1.0 + w_norm.astype(jnp.float32))).astype(jnp.bfloat16)
    q_proj = jnp.dot(x_norm, w_q, preferred_element_type=jnp.float32).astype(jnp.bfloat16)
    k_proj = jnp.dot(x_norm, w_k, preferred_element_type=jnp.float32).astype(jnp.bfloat16)
    v_proj = jnp.dot(x_norm, w_v, preferred_element_type=jnp.float32).astype(jnp.bfloat16)
    inv_freq = ROPE_BASE ** (-jnp.arange(HEAD // 2, dtype=jnp.float32) * 2.0 / HEAD)
    angles = cache_len.astype(jnp.float32)[:, None] * inv_freq[None, :]
    cos_t = jnp.cos(angles)
    sin_t = jnp.sin(angles)
    q_heads = q_proj.astype(jnp.float32).reshape(ROWS, HEADS, HEAD)
    q_rot = (rotate_half(q_heads, cos_t[:, None, :], sin_t[:, None, :]) * HEAD ** -0.5).astype(jnp.bfloat16)
    k_rot = rotate_half(k_proj.astype(jnp.float32), cos_t, sin_t).astype(jnp.bfloat16)
    positions = jnp.arange(SEQ)
    at_slot = (positions[None, :] == cache_len[:, None])[:, :, None]
    new_k_cache = jnp.where(at_slot, k_rot[:, None, :], k_cache)
    new_v_cache = jnp.where(at_slot, v_proj[:, None, :], v_cache)

    def one_row(row_args):
        q_row, k_row, v_row, length = row_args
        scores = jnp.einsum('hd,td->ht', q_row.astype(jnp.float32), k_row.astype(jnp.float32))
        scores = jnp.where(positions[None, :] <= length, scores, -jnp.inf)
        weights = jax.nn.softmax(scores, axis=-1)
        return jnp.einsum('ht,td->hd', weights, v_row.astype(jnp.float32))

    attended = lax.map(one_row, (q_rot, new_k_cache, new_v_cache, cache_len))
    attended = attended.reshape(ROWS, HEADS * HEAD).astype(jnp.bfloat16)
    out_hidden = x_f32 + jnp.dot(attended, w_o, preferred_element_type=jnp.float32)
    return out_hidden.astype(jnp.bfloat16), new_k_cache, new_v_cache
```

```python
import functools

import jax
import jax.numpy as jnp
from jax import lax
from jax.experimental import pallas as pl
from jax.experimental.pallas import tpu as pltpu
from jax.sharding import PartitionSpec as P

ROPE_BASE = 10000.0
EPSILON = 1e-6
MESH = pl.DeviceIdType.MESH
MIB = 1 << 20
LOWEST = float(jnp.finfo(jnp.float32).min)
CHIPS = 4


def rotate(x, cos_t, sin_t):
    half = x.shape[-1] // 2
    low, high = x[:, :half], x[:, half:]
    return jnp.concatenate([low * cos_t - high * sin_t, high * cos_t + low * sin_t], axis=-1)


def project_kernel(hid_ref, wn_ref, cos_ref, sin_ref, wk_hbm, wv_hbm, wq_hbm, q_ref, k_ref, v_ref,
                   xn, wk, wv, wq, sem_k, sem_v, sem_q):
    rows, head_dim = hid_ref.shape[0], wk.shape[1]
    heads, half = wq.shape[0], head_dim // 2
    brows = rows // q_ref.shape[0]
    core = lax.rem(lax.axis_index('sp'), 2)

    def q_copy(j):
        columns = pl.ds(pl.multiple_of((core * heads + j) * head_dim, head_dim), head_dim)
        return pltpu.make_async_copy(wq_hbm.at[:, columns], wq.at[j], sem_q.at[j])

    k_copy = pltpu.make_async_copy(wk_hbm, wk, sem_k)
    v_copy = pltpu.make_async_copy(wv_hbm, wv, sem_v)
    k_copy.start()
    v_copy.start()
    for j in range(heads):
        q_copy(j).start()
    x = hid_ref[...].astype(jnp.float32)
    inv_rms = lax.rsqrt(jnp.mean(x * x, axis=-1, keepdims=True) + EPSILON)
    xn[...] = (x * inv_rms * (1.0 + wn_ref[...].astype(jnp.float32))).astype(jnp.bfloat16)
    cos_t, sin_t = cos_ref[...], sin_ref[...]

    def project(w):
        y = jnp.dot(xn[...], w, preferred_element_type=jnp.float32)
        return y.astype(jnp.bfloat16)

    k_copy.wait()
    k_ref[...] = rotate(project(wk[...]).astype(jnp.float32), cos_t, sin_t).astype(jnp.bfloat16)
    v_copy.wait()
    v_ref[...] = project(wv[...])

    def one_head(j, carry):
        q_copy(j).wait()
        y = project(wq[j]).astype(jnp.float32)
        y = (rotate(y, cos_t, sin_t) * head_dim ** -0.5).astype(jnp.bfloat16).astype(jnp.float32)
        for i in range(q_ref.shape[0]):
            for d in range(2):
                q_ref[i, d, pl.ds(j, brows, stride=heads), :] = y[i * brows:(i + 1) * brows, d * half:(d + 1) * half]
        return carry

    lax.fori_loop(0, heads, one_head, 0)


def attend_kernel(len_ref, qh_ref, kc_ref, vc_ref, hid_ref, wo_hbm, out_ref,
                  q_all, p_buf, num, stat_src, stat_dst, d_recv, s_sum, r_recv, l_recv, from_left, from_right,
                  att, a_bf, wo, gath, other,
                  sem_wo, sem_ql, q_s, q_r, st_s, st_r, d_s, d_r, rs_s, rs_r, at_s, at_r,
                  own_s, own_r, fw_s, fw_r, h_s, h_r):
    f32, bf16 = jnp.float32, jnp.bfloat16
    me = lax.axis_index('sp')
    chip, core = me // 2, lax.rem(me, 2)
    mate = 1 - core
    peers = 2 * CHIPS
    slots = kc_ref.shape[1]
    nblk, brows = num.shape[0], kc_ref.shape[0] // num.shape[0]
    heads = num.shape[2] // brows
    hh = heads // 2
    hl = num.shape[3]
    hd = 2 * hl
    nq = wo.shape[0]

    def at(c, k):
        return {'sp': lax.rem(c + CHIPS, CHIPS) * 2 + k}

    right, left = at(chip + 1, core), at(chip - 1, core)
    partner = at(chip, mate)

    def remote(src, dst, ssem, rsem, dev):
        return pltpu.make_async_remote_copy(src_ref=src, dst_ref=dst, send_sem=ssem, recv_sem=rsem,
                                            device_id=dev, device_id_type=MESH)

    def wo_copy(j):
        columns = pl.ds(pl.multiple_of((core * nq + j) * hd, hd), hd)
        return pltpu.make_async_copy(wo_hbm.at[:, columns], wo.at[j], sem_wo.at[j])

    for j in range(nq):
        wo_copy(j).start()

    barrier = pltpu.get_barrier_semaphore()
    for d in range(1, peers):
        pl.semaphore_signal(barrier, inc=1, device_id={'sp': lax.rem(me + d, peers)}, device_id_type=MESH)
    pl.semaphore_wait(barrier, peers - 1)

    nqc = q_s.shape[0]
    per = nblk // nqc
    q_sends, q_local = [], []
    for t in range(nqc):
        part = pl.ds(t * per, per)
        copy = remote(qh_ref.at[part], q_all.at[core, part], q_s.at[t], q_r.at[t], partner)
        copy.start()
        q_sends.append(copy)
        copy = pltpu.make_async_copy(qh_ref.at[part], q_all.at[core, part], sem_ql.at[t])
        copy.start()
        q_local.append(copy)

    lane = lax.broadcasted_iota(jnp.int32, (heads, slots), 1)
    position = me * slots + lane

    def scores(i, kk):
        c = i // 2
        stat = stat_src[kk]
        base = c * brows
        for r in range(brows):
            b = i * brows + r
            own_rows = slice(r * hh, (r + 1) * hh)
            q = jnp.concatenate([
                jnp.concatenate([q_all[k, i, d, own_rows, :] for k in range(2)], axis=0) for d in range(2)], axis=1)
            s = lax.dot_general(q.astype(bf16), kc_ref[b], (((1,), (1,)), ((), ())), preferred_element_type=f32)
            valid = position <= len_ref[b]
            s = jnp.where(valid, s, LOWEST)
            m = jnp.max(s, axis=1, keepdims=True)
            p = jnp.where(valid, jnp.exp(s - m), 0.0)
            p_buf[b] = p.astype(bf16)
            den = jnp.sum(p, axis=1, keepdims=True)
            stat = jnp.where(lane == base + r, m, jnp.where(lane == slots // 2 + base + r, den, stat))
        stat_src[kk] = stat

    stat_src[...] = jnp.zeros_like(stat_src)
    for t in range(nqc):
        q_local[t].wait()
        q_sends[t].wait_recv()

        def pair(u, carry):
            i = t * per + u
            scores(i, lax.rem(i, 2))
            return carry

        lax.fori_loop(0, per, pair, 0)

    st_sends = []
    for d in range(1, peers):
        target = lax.rem(me + d, peers)
        copy = remote(stat_src.at[lax.rem(target, 2)], stat_dst.at[d - 1], st_s.at[d - 1], st_r.at[d - 1],
                      {'sp': target})
        copy.start()
        st_sends.append(copy)

    def values(i):
        for r in range(brows):
            b = i * brows + r
            o = jnp.dot(p_buf[b], vc_ref[b], preferred_element_type=f32)
            for d in range(2):
                num[i, d, r * heads:(r + 1) * heads, :] = o[:, d * hl:(d + 1) * hl]

    offsets = (2, 1, 3, 0)
    places = [lax.rem(chip + o, CHIPS) for o in offsets]
    d_sends = []
    for t in range(CHIPS):
        values(2 * places[t] + mate)
        copy = remote(num.at[2 * places[t] + mate], d_recv.at[t], d_s.at[t], d_r.at[t], partner)
        copy.start()
        d_sends.append(copy)
        values(2 * places[t] + core)

    for copy in st_sends:
        copy.wait_recv()
    mine = stat_src[core]
    theirs = [stat_dst[d] for d in range(peers - 1)]
    top = functools.reduce(jnp.maximum, theirs, mine)
    half = slots // 2
    mate_d = jnp.where(core == 1, 0, peers - 2)
    own_a = jnp.exp(mine - top)
    total = own_a * pltpu.roll(mine, half, 1)
    for x in theirs:
        total = total + jnp.exp(x - top) * pltpu.roll(x, half, 1)
    in_use = lane < half
    total = jnp.where(in_use, total, 1.0)
    f_own = jnp.where(in_use, own_a, 0.0) / total
    f_mate = jnp.where(in_use, jnp.exp(stat_dst[mate_d] - top), 0.0) / total

    def combine(t):
        d_sends[t].wait_recv()
        shift = slots - places[t] * brows
        fo, fm = pltpu.roll(f_own, shift, 1), pltpu.roll(f_mate, shift, 1)
        i = 2 * places[t] + core
        for r in range(brows):
            part = pl.ds(r * heads, heads)
            for d in range(2):
                s_sum[t, d, part, :] = num[i, d, part, :] * fo[:, r:r + 1] + d_recv[t, d, part, :] * fm[:, r:r + 1]

    def ring(n, src, dst, dev):
        copy = remote(src, dst, rs_s.at[n], rs_r.at[n], dev)
        copy.start()
        return copy

    combine(0)
    r1 = ring(0, s_sum.at[0, 0], r_recv, right)
    l1 = ring(1, s_sum.at[0, 1], l_recv, left)
    combine(1)
    r2a = ring(2, s_sum.at[1, 1], from_left.at[1], right)
    combine(2)
    l2a = ring(3, s_sum.at[2, 0], from_right.at[0], left)
    r1.wait_recv()
    s_sum[1, 0] = s_sum[1, 0] + r_recv[...]
    r2b = ring(4, s_sum.at[1, 0], from_left.at[0], right)
    l1.wait_recv()
    s_sum[2, 1] = s_sum[2, 1] + l_recv[...]
    l2b = ring(5, s_sum.at[2, 1], from_right.at[1], left)
    combine(3)
    for copy in (r2a, r2b, l2a, l2b):
        copy.wait_recv()
    att[core] = s_sum[3] + from_left[...] + from_right[...]
    at_copy = remote(att.at[core], att.at[core], at_s, at_r, partner)
    at_copy.start()
    at_copy.wait_recv()

    for h in range(heads):
        for d in range(2):
            pair = [att[kk, d, pl.ds(h, brows, stride=heads), :] for kk in range(2)]
            a_bf[:, h * hd + d * hl:h * hd + (d + 1) * hl] = jnp.concatenate(pair, axis=0).astype(bf16)
    crow = 2 * brows

    def own_copies(n):
        piece = gath.at[chip, n]
        return (remote(piece, piece, own_s.at[0, n], own_r.at[0, n], right),
                remote(piece, piece, own_s.at[1, n], own_r.at[1, n], left),
                remote(piece, other.at[chip, n], h_s.at[0, n], h_r.at[0, n], partner))

    def rows_of(c):
        return pl.ds(pl.multiple_of(c * crow, crow), crow)

    def columns_of(k, n):
        return pl.ds(pl.multiple_of((k * nq + n) * hd, hd), hd)

    def project(n, carry):
        wo_copy(n).wait()
        y = jnp.dot(a_bf[...], wo[n], preferred_element_type=f32)
        x = hid_ref[rows_of(chip), columns_of(core, n)].astype(f32)
        gath[chip, n] = x + y
        for copy in own_copies(n):
            copy.start()
        return carry

    lax.fori_loop(0, nq, project, 0)

    cl, cr, co = places[2], places[1], places[0]
    fsplit = nq // 2

    def forward(n):
        if n < fsplit:
            return remote(gath.at[cl, n], gath.at[cl, n], fw_s.at[n], fw_r.at[n], right)
        return remote(gath.at[cr, n], gath.at[cr, n], fw_s.at[n], fw_r.at[n], left)

    def to_mate(which, c, n):
        return remote(gath.at[c, n], other.at[c, n], h_s.at[which, n], h_r.at[which, n], partner)

    def put(c, n):
        out_ref[rows_of(c), columns_of(core, n)] = gath[c, n].astype(bf16)

    for n in range(nq):
        from_l, from_r, _ = own_copies(n)
        from_l.wait_recv()
        if n < fsplit:
            forward(n).start()
        to_mate(1, cl, n).start()
        from_r.wait_recv()
        if n >= fsplit:
            forward(n).start()
        to_mate(2, cr, n).start()
    for n in range(nq):
        put(chip, n)
        put(cl, n)
        put(cr, n)
    for n in range(nq):
        forward(n).wait_recv()
        to_mate(3, co, n).start()
        put(co, n)
    for which, c in enumerate((chip, cl, cr, co)):
        for n in range(nq):
            to_mate(which, c, n).wait_recv()
            out_ref[rows_of(c), columns_of(mate, n)] = other[c, n].astype(bf16)

    for copy in q_sends + st_sends + d_sends + [r1, l1, r2a, l2a, r2b, l2b, at_copy]:
        copy.wait_send()
    for n in range(nq):
        for copy in own_copies(n):
            copy.wait_send()
        forward(n).wait_send()
        for which, c in ((1, cl), (2, cr), (3, co)):
            to_mate(which, c, n).wait_send()


def local_step(hidden, w_norm, w_q, w_k, w_v, w_o, k_block, v_block, cache_len):
    f32, bf16 = jnp.float32, jnp.bfloat16
    rows, width = hidden.shape
    seq_block, hd = k_block.shape[1], k_block.shape[2]
    heads = w_q.shape[1] // hd
    hh = heads // 2
    nblk = 2 * CHIPS
    brows = rows // nblk
    inv_freq = ROPE_BASE ** (-jnp.arange(hd // 2, dtype=f32) * 2.0 / hd)
    angles = cache_len.astype(f32)[:, None] * inv_freq[None, :]
    cos_t, sin_t = jnp.cos(angles), jnp.sin(angles)
    vmem = pl.BlockSpec(memory_space=pltpu.VMEM)
    hbm = pl.BlockSpec(memory_space=pl.ANY)
    smem = pl.BlockSpec(memory_space=pltpu.SMEM)
    dma = pltpu.SemaphoreType.DMA

    qh, k_rot, v_new = pl.pallas_call(
        project_kernel,
        out_shape=(jax.ShapeDtypeStruct((nblk, 2, brows * hh, hd // 2), f32), jax.ShapeDtypeStruct((rows, hd), bf16),
                   jax.ShapeDtypeStruct((rows, hd), bf16)),
        in_specs=[vmem] * 4 + [hbm] * 3,
        out_specs=(vmem,) * 3,
        scratch_shapes=[
            pltpu.VMEM((rows, width), bf16),
            pltpu.VMEM((width, hd), bf16),
            pltpu.VMEM((width, hd), bf16),
            pltpu.VMEM((hh, width, hd), bf16),
            dma, dma, dma((hh,)),
        ],
        compiler_params=pltpu.CompilerParams(vmem_limit_bytes=28 * MIB),
        cost_estimate=pl.CostEstimate(flops=2 * rows * width * (hh + 2) * hd, bytes_accessed=2 * width * (hh + 2) * hd,
                                      transcendentals=0),
        name='project',
    )(hidden, w_norm.reshape(1, width), cos_t, sin_t, w_k, w_v, w_q)

    positions = lax.axis_index('sp') * seq_block + jnp.arange(seq_block)
    at_slot = (positions[None, :] == cache_len[:, None])[:, :, None]
    new_k_block = jnp.where(at_slot, k_rot[:, None, :], k_block)
    new_v_block = jnp.where(at_slot, v_new[:, None, :], v_block)

    block, hl = brows * heads, hd // 2
    nqc = CHIPS
    out_hidden = pl.pallas_call(
        attend_kernel,
        out_shape=jax.ShapeDtypeStruct((rows, width), bf16),
        in_specs=[smem, vmem, vmem, vmem, vmem, hbm],
        out_specs=vmem,
        scratch_shapes=[
            pltpu.VMEM((2, nblk, 2, brows * hh, hl), f32),
            pltpu.VMEM((rows, heads, seq_block), bf16),
            pltpu.VMEM((nblk, 2, block, hl), f32),
            pltpu.VMEM((2, heads, seq_block), f32),
            pltpu.VMEM((nblk - 1, heads, seq_block), f32),
            pltpu.VMEM((CHIPS, 2, block, hl), f32),
            pltpu.VMEM((CHIPS, 2, block, hl), f32),
            pltpu.VMEM((block, hl), f32),
            pltpu.VMEM((block, hl), f32),
            pltpu.VMEM((2, block, hl), f32),
            pltpu.VMEM((2, block, hl), f32),
            pltpu.VMEM((2, 2, block, hl), f32),
            pltpu.VMEM((2 * brows, width), bf16),
            pltpu.VMEM((hh, width, hd), bf16),
            pltpu.VMEM((CHIPS, hh, 2 * brows, hd), f32),
            pltpu.VMEM((CHIPS, hh, 2 * brows, hd), f32),
            dma((hh,)), dma((nqc,)), dma((nqc,)), dma((nqc,)), dma((nblk - 1,)), dma((nblk - 1,)),
            dma((CHIPS,)), dma((CHIPS,)), dma((6,)), dma((6,)), dma, dma,
            dma((2, hh)), dma((2, hh)), dma((hh,)), dma((hh,)), dma((CHIPS, hh)), dma((CHIPS, hh)),
        ],
        compiler_params=pltpu.CompilerParams(collective_id=0, has_side_effects=True, vmem_limit_bytes=34 * MIB),
        cost_estimate=pl.CostEstimate(flops=2 * rows * width * hh * hd * 2, bytes_accessed=2 * width * hh * hd,
                                      transcendentals=0),
        name='attend',
    )(cache_len, qh, new_k_block, new_v_block, hidden, w_o)
    return out_hidden, new_k_block, new_v_block


def solution(mesh):
    assert mesh.shape['sp'] == 2 * CHIPS
    cache_spec = P('dp', 'sp', None)
    return jax.shard_map(local_step, mesh=mesh, in_specs=(P('dp', None), P(None), P(None, None), P(None, None), P(None, None), P(None, None), cache_spec, cache_spec, P('dp')), out_specs=(P('dp', None), cache_spec, cache_spec), check_vma=False)
```

```python
import functools

import jax
import jax.numpy as jnp
from jax import lax
from jax.experimental import pallas as pl
from jax.experimental.pallas import tpu as pltpu
from jax.sharding import PartitionSpec as P

ROPE_BASE = 10000.0
EPSILON = 1e-6
MESH = pl.DeviceIdType.MESH
MIB = 1 << 20
LOWEST = float(jnp.finfo(jnp.float32).min)
CHIPS = 4


def rotate(x, cos_t, sin_t):
    half = x.shape[-1] // 2
    low, high = x[:, :half], x[:, half:]
    return jnp.concatenate([low * cos_t - high * sin_t, high * cos_t + low * sin_t], axis=-1)


def project_kernel(len_ref, hid_hbm, wn_ref, wk_hbm, wv_hbm, wq_hbm, kc_hbm, vc_hbm, q_ref, k_ref, v_ref, slot_ref,
                   kc, vc, hid, xn, wk, wv, wq, mine, theirs, sem_h, sem_k, sem_v, sem_q, sem_c, x_s, x_r):
    f32, bf16 = jnp.float32, jnp.bfloat16
    rows, width = hid.shape
    head_dim = wk.shape[1]
    heads, half = wq.shape[0], head_dim // 2
    brows = rows // q_ref.shape[1]
    me = lax.axis_index('sp')
    core = lax.rem(me, 2)
    partner = {'sp': me + 1 - 2 * core}

    def q_copy(j):
        columns = pl.ds(pl.multiple_of((core * heads + j) * head_dim, head_dim), head_dim)
        return pltpu.make_async_copy(wq_hbm.at[:, columns], wq.at[j], sem_q.at[j])

    crows = kc.shape[0] // heads

    def cache_copies(j):
        part = pl.ds(j * crows, crows)
        return (pltpu.make_async_copy(kc_hbm.at[part], kc.at[part], sem_c.at[0, j]),
                pltpu.make_async_copy(vc_hbm.at[part], vc.at[part], sem_c.at[1, j]))

    def exchange(j):
        return pltpu.make_async_remote_copy(src_ref=mine.at[j], dst_ref=theirs.at[j], send_sem=x_s.at[j],
                                            recv_sem=x_r.at[j], device_id=partner, device_id_type=MESH)

    h_copy = pltpu.make_async_copy(hid_hbm, hid, sem_h)
    k_copy = pltpu.make_async_copy(wk_hbm, wk, sem_k)
    v_copy = pltpu.make_async_copy(wv_hbm, wv, sem_v)
    h_copy.start()
    k_copy.start()
    v_copy.start()
    for j in range(heads):
        q_copy(j).start()
    barrier = pltpu.get_barrier_semaphore()
    pl.semaphore_signal(barrier, inc=1, device_id=partner, device_id_type=MESH)

    lengths = len_ref[...].reshape(1, rows)
    across = lax.broadcasted_iota(jnp.int32, (rows, rows), 1)
    down = lax.broadcasted_iota(jnp.int32, (rows, rows), 0)
    column = jnp.sum(jnp.where(across == down, lengths, 0).astype(f32), axis=1, keepdims=True)
    slots = slot_ref.shape[1]
    slot = lax.broadcasted_iota(jnp.int32, (rows, slots), 1) + me * slots
    slot_ref[...] = (slot.astype(f32) == column).astype(jnp.int32)
    angles = column * wn_ref[0:1, width:width + half]
    cos_t, sin_t = jnp.cos(angles), jnp.sin(angles)

    h_copy.wait()
    x = hid[...].astype(f32)
    inv_rms = lax.rsqrt(jnp.mean(x * x, axis=-1, keepdims=True) + EPSILON)
    xn[...] = (x * inv_rms * (1.0 + wn_ref[:, 0:width])).astype(bf16)

    def project(w):
        y = jnp.dot(xn[...], w, preferred_element_type=f32)
        return y.astype(bf16)

    k_copy.wait()
    k_ref[...] = rotate(project(wk[...]).astype(f32), cos_t, sin_t).astype(bf16)
    v_copy.wait()
    v_ref[...] = project(wv[...])
    pl.semaphore_wait(barrier, 1)

    def place(k, j, y):
        for i in range(q_ref.shape[1]):
            for d in range(2):
                q_ref[k, i, d, pl.ds(j, brows, stride=heads), :] = y[i * brows:(i + 1) * brows, d * half:(d + 1) * half]

    def one_head(j, carry):
        q_copy(j).wait()
        for copy in cache_copies(j):
            copy.start()
        y = project(wq[j]).astype(f32)
        mine[j] = (rotate(y, cos_t, sin_t) * head_dim ** -0.5).astype(bf16).astype(f32)
        exchange(j).start()
        place(core, j, mine[j])
        return carry

    lax.fori_loop(0, heads, one_head, 0)

    def their_head(j, carry):
        exchange(j).wait_recv()
        place(1 - core, j, theirs[j])
        return carry

    lax.fori_loop(0, heads, their_head, 0)

    def finish(j, carry):
        exchange(j).wait_send()
        for copy in cache_copies(j):
            copy.wait()
        return carry

    lax.fori_loop(0, heads, finish, 0)


def attend_kernel(len_ref, q_all, kc_ref, vc_ref, hid_ref, wo_hbm, out_ref,
                  p_buf, num, stat_src, stat_dst, d_recv, s_sum, r_recv, l_recv, from_left, from_right,
                  att, a_bf, wo, gath, other,
                  sem_wo, st_s, st_r, d_s, d_r, rs_s, rs_r, at_s, at_r,
                  own_s, own_r, fw_s, fw_r, h_s, h_r):
    f32, bf16 = jnp.float32, jnp.bfloat16
    me = lax.axis_index('sp')
    chip, core = me // 2, lax.rem(me, 2)
    mate = 1 - core
    peers = 2 * CHIPS
    slots = kc_ref.shape[1]
    nblk, brows = num.shape[0], kc_ref.shape[0] // num.shape[0]
    heads = num.shape[2] // brows
    hh = heads // 2
    hl = num.shape[3]
    hd = 2 * hl
    nq = wo.shape[0]

    def at(c, k):
        return {'sp': lax.rem(c + CHIPS, CHIPS) * 2 + k}

    right, left = at(chip + 1, core), at(chip - 1, core)
    partner = at(chip, mate)

    def remote(src, dst, ssem, rsem, dev):
        return pltpu.make_async_remote_copy(src_ref=src, dst_ref=dst, send_sem=ssem, recv_sem=rsem,
                                            device_id=dev, device_id_type=MESH)

    def wo_copy(j):
        columns = pl.ds(pl.multiple_of((core * nq + j) * hd, hd), hd)
        return pltpu.make_async_copy(wo_hbm.at[:, columns], wo.at[j], sem_wo.at[j])

    barrier = pltpu.get_barrier_semaphore()
    for d in range(1, peers):
        pl.semaphore_signal(barrier, inc=1, device_id={'sp': lax.rem(me + d, peers)}, device_id_type=MESH)
    lane = lax.broadcasted_iota(jnp.int32, (heads, slots), 1)
    position = me * slots + lane

    def scores(i, kk):
        c = i // 2
        stat = stat_src[kk]
        base = c * brows
        for r in range(brows):
            b = i * brows + r
            own_rows = slice(r * hh, (r + 1) * hh)
            q = jnp.concatenate([
                jnp.concatenate([q_all[k, i, d, own_rows, :] for k in range(2)], axis=0) for d in range(2)], axis=1)
            s = lax.dot_general(q.astype(bf16), kc_ref[b], (((1,), (1,)), ((), ())), preferred_element_type=f32)
            valid = position <= len_ref[b]
            s = jnp.where(valid, s, LOWEST)
            m = jnp.max(s, axis=1, keepdims=True)
            p = jnp.where(valid, jnp.exp(s - m), 0.0)
            p_buf[b] = p.astype(bf16)
            den = jnp.sum(p, axis=1, keepdims=True)
            stat = jnp.where(lane == base + r, m, jnp.where(lane == slots // 2 + base + r, den, stat))
        stat_src[kk] = stat

    stat_src[...] = jnp.zeros_like(stat_src)

    def block_scores(i, carry):
        scores(i, lax.rem(i, 2))
        return carry

    lax.fori_loop(0, nblk, block_scores, 0)
    pl.semaphore_wait(barrier, peers - 1)

    st_sends = []
    for d in range(1, peers):
        target = lax.rem(me + d, peers)
        copy = remote(stat_src.at[lax.rem(target, 2)], stat_dst.at[d - 1], st_s.at[d - 1], st_r.at[d - 1],
                      {'sp': target})
        copy.start()
        st_sends.append(copy)

    def values(i):
        for r in range(brows):
            b = i * brows + r
            o = jnp.dot(p_buf[b], vc_ref[b], preferred_element_type=f32)
            for d in range(2):
                num[i, d, r * heads:(r + 1) * heads, :] = o[:, d * hl:(d + 1) * hl]

    offsets = (2, 1, 3, 0)
    places = [lax.rem(chip + o, CHIPS) for o in offsets]
    d_sends = []
    for t in range(CHIPS):
        values(2 * places[t] + mate)
        copy = remote(num.at[2 * places[t] + mate], d_recv.at[t], d_s.at[t], d_r.at[t], partner)
        copy.start()
        d_sends.append(copy)
        values(2 * places[t] + core)

    for j in range(nq):
        wo_copy(j).start()
    for copy in st_sends:
        copy.wait_recv()
    mine = stat_src[core]
    theirs = [stat_dst[d] for d in range(peers - 1)]
    top = functools.reduce(jnp.maximum, theirs, mine)
    half = slots // 2
    mate_d = jnp.where(core == 1, 0, peers - 2)
    own_a = jnp.exp(mine - top)
    total = own_a * pltpu.roll(mine, half, 1)
    for x in theirs:
        total = total + jnp.exp(x - top) * pltpu.roll(x, half, 1)
    in_use = lane < half
    total = jnp.where(in_use, total, 1.0)
    f_own = jnp.where(in_use, own_a, 0.0) / total
    f_mate = jnp.where(in_use, jnp.exp(stat_dst[mate_d] - top), 0.0) / total

    def combine(t):
        d_sends[t].wait_recv()
        shift = slots - places[t] * brows
        fo, fm = pltpu.roll(f_own, shift, 1), pltpu.roll(f_mate, shift, 1)
        i = 2 * places[t] + core
        for r in range(brows):
            part = pl.ds(r * heads, heads)
            for d in range(2):
                s_sum[t, d, part, :] = num[i, d, part, :] * fo[:, r:r + 1] + d_recv[t, d, part, :] * fm[:, r:r + 1]

    def ring(n, src, dst, dev):
        copy = remote(src, dst, rs_s.at[n], rs_r.at[n], dev)
        copy.start()
        return copy

    combine(0)
    r1 = ring(0, s_sum.at[0, 0], r_recv, right)
    l1 = ring(1, s_sum.at[0, 1], l_recv, left)
    combine(1)
    r2a = ring(2, s_sum.at[1, 1], from_left.at[1], right)
    combine(2)
    l2a = ring(3, s_sum.at[2, 0], from_right.at[0], left)
    r1.wait_recv()
    s_sum[1, 0] = s_sum[1, 0] + r_recv[...]
    r2b = ring(4, s_sum.at[1, 0], from_left.at[0], right)
    l1.wait_recv()
    s_sum[2, 1] = s_sum[2, 1] + l_recv[...]
    l2b = ring(5, s_sum.at[2, 1], from_right.at[1], left)
    combine(3)
    for copy in (r2a, r2b, l2a, l2b):
        copy.wait_recv()
    att[core] = s_sum[3] + from_left[...] + from_right[...]
    at_copy = remote(att.at[core], att.at[core], at_s, at_r, partner)
    at_copy.start()
    at_copy.wait_recv()

    for h in range(heads):
        for d in range(2):
            pair = [att[kk, d, pl.ds(h, brows, stride=heads), :] for kk in range(2)]
            a_bf[:, h * hd + d * hl:h * hd + (d + 1) * hl] = jnp.concatenate(pair, axis=0).astype(bf16)
    crow = 2 * brows

    def own_copies(n):
        piece = gath.at[chip, n]
        return (remote(piece, piece, own_s.at[0, n], own_r.at[0, n], right),
                remote(piece, piece, own_s.at[1, n], own_r.at[1, n], left),
                remote(piece, other.at[chip, n], h_s.at[0, n], h_r.at[0, n], partner))

    def rows_of(c):
        return pl.ds(pl.multiple_of(c * crow, crow), crow)

    def columns_of(k, n):
        return pl.ds(pl.multiple_of((k * nq + n) * hd, hd), hd)

    def project(n, carry):
        wo_copy(n).wait()
        y = jnp.dot(a_bf[...], wo[n], preferred_element_type=f32)
        x = hid_ref[rows_of(chip), columns_of(core, n)].astype(f32)
        gath[chip, n] = x + y
        for copy in own_copies(n):
            copy.start()
        return carry

    lax.fori_loop(0, nq, project, 0)

    cl, cr, co = places[2], places[1], places[0]
    fsplit = nq // 2

    def forward(n):
        if n < fsplit:
            return remote(gath.at[cl, n], gath.at[cl, n], fw_s.at[n], fw_r.at[n], right)
        return remote(gath.at[cr, n], gath.at[cr, n], fw_s.at[n], fw_r.at[n], left)

    def to_mate(which, c, n):
        return remote(gath.at[c, n], other.at[c, n], h_s.at[which, n], h_r.at[which, n], partner)

    def put(c, n):
        out_ref[rows_of(c), columns_of(core, n)] = gath[c, n].astype(bf16)

    for n in range(nq):
        from_l, from_r, _ = own_copies(n)
        from_l.wait_recv()
        if n < fsplit:
            forward(n).start()
        to_mate(1, cl, n).start()
        from_r.wait_recv()
        if n >= fsplit:
            forward(n).start()
        to_mate(2, cr, n).start()
    for n in range(nq):
        put(chip, n)
        put(cl, n)
        put(cr, n)
    for n in range(nq):
        forward(n).wait_recv()
        to_mate(3, co, n).start()
        put(co, n)
    for which, c in enumerate((chip, cl, cr, co)):
        for n in range(nq):
            to_mate(which, c, n).wait_recv()
            out_ref[rows_of(c), columns_of(mate, n)] = other[c, n].astype(bf16)

    for copy in st_sends + d_sends + [r1, l1, r2a, l2a, r2b, l2b, at_copy]:
        copy.wait_send()
    for n in range(nq):
        for copy in own_copies(n):
            copy.wait_send()
        forward(n).wait_send()
        for which, c in ((1, cl), (2, cr), (3, co)):
            to_mate(which, c, n).wait_send()


def local_step(hidden, w_norm, w_q, w_k, w_v, w_o, k_block, v_block, cache_len):
    f32, bf16 = jnp.float32, jnp.bfloat16
    rows, width = hidden.shape
    seq_block, hd = k_block.shape[1], k_block.shape[2]
    heads = w_q.shape[1] // hd
    hh = heads // 2
    nblk = 2 * CHIPS
    brows = rows // nblk
    inv_freq = ROPE_BASE ** (-jnp.arange(hd // 2, dtype=f32) * 2.0 / hd)
    gain_freq = jnp.concatenate([w_norm.astype(f32), inv_freq]).reshape(1, width + hd // 2)
    vmem = pl.BlockSpec(memory_space=pltpu.VMEM)
    hbm = pl.BlockSpec(memory_space=pl.ANY)
    smem = pl.BlockSpec(memory_space=pltpu.SMEM)
    dma = pltpu.SemaphoreType.DMA

    def keep(x):
        return pltpu.with_memory_space_constraint(x, pltpu.HBM)

    def near(x):
        return pltpu.with_memory_space_constraint(x, pltpu.VMEM)

    q_all, k_rot, v_new, slot, k_near, v_near = pl.pallas_call(
        project_kernel,
        out_shape=(pltpu.VMEM((2, nblk, 2, brows * hh, hd // 2), f32), jax.ShapeDtypeStruct((rows, hd), bf16),
                   jax.ShapeDtypeStruct((rows, hd), bf16), jax.ShapeDtypeStruct((rows, seq_block), jnp.int32),
                   pltpu.VMEM(k_block.shape, bf16), pltpu.VMEM(v_block.shape, bf16)),
        in_specs=[vmem, hbm, vmem] + [hbm] * 5,
        out_specs=(vmem,) * 6,
        scratch_shapes=[
            pltpu.VMEM((rows, width), bf16),
            pltpu.VMEM((rows, width), bf16),
            pltpu.VMEM((width, hd), bf16),
            pltpu.VMEM((width, hd), bf16),
            pltpu.VMEM((hh, width, hd), bf16),
            pltpu.VMEM((hh, rows, hd), f32),
            pltpu.VMEM((hh, rows, hd), f32),
            dma, dma, dma, dma((hh,)), dma((2, hh)), dma((hh,)), dma((hh,)),
        ],
        compiler_params=pltpu.CompilerParams(collective_id=1, has_side_effects=True, vmem_limit_bytes=27 * MIB),
        cost_estimate=pl.CostEstimate(flops=2 * rows * width * (hh + 2) * hd, bytes_accessed=2 * width * (hh + 2) * hd,
                                      transcendentals=0),
        name='project',
    )(cache_len, keep(hidden), gain_freq, keep(w_k), keep(w_v), keep(w_q), keep(k_block), keep(v_block))

    at_slot = (slot != 0)[:, :, None]
    new_k_block = jnp.where(at_slot, k_rot[:, None, :], k_near)
    new_k_block, v_near = lax.optimization_barrier((new_k_block, v_near))
    new_v_block = jnp.where(at_slot, v_new[:, None, :], v_near)

    block, hl = brows * heads, hd // 2
    out_hidden = pl.pallas_call(
        attend_kernel,
        out_shape=jax.ShapeDtypeStruct((rows, width), bf16),
        in_specs=[smem, vmem, vmem, vmem, vmem, hbm],
        out_specs=vmem,
        scratch_shapes=[
            pltpu.VMEM((rows, heads, seq_block), bf16),
            pltpu.VMEM((nblk, 2, block, hl), f32),
            pltpu.VMEM((2, heads, seq_block), f32),
            pltpu.VMEM((nblk - 1, heads, seq_block), f32),
            pltpu.VMEM((CHIPS, 2, block, hl), f32),
            pltpu.VMEM((CHIPS, 2, block, hl), f32),
            pltpu.VMEM((block, hl), f32),
            pltpu.VMEM((block, hl), f32),
            pltpu.VMEM((2, block, hl), f32),
            pltpu.VMEM((2, block, hl), f32),
            pltpu.VMEM((2, 2, block, hl), f32),
            pltpu.VMEM((2 * brows, width), bf16),
            pltpu.VMEM((hh, width, hd), bf16),
            pltpu.VMEM((CHIPS, hh, 2 * brows, hd), f32),
            pltpu.VMEM((CHIPS, hh, 2 * brows, hd), f32),
            dma((hh,)), dma((nblk - 1,)), dma((nblk - 1,)),
            dma((CHIPS,)), dma((CHIPS,)), dma((6,)), dma((6,)), dma, dma,
            dma((2, hh)), dma((2, hh)), dma((hh,)), dma((hh,)), dma((CHIPS, hh)), dma((CHIPS, hh)),
        ],
        compiler_params=pltpu.CompilerParams(collective_id=0, has_side_effects=True, vmem_limit_bytes=27 * MIB),
        cost_estimate=pl.CostEstimate(flops=2 * rows * width * hh * hd * 2, bytes_accessed=2 * width * hh * hd,
                                      transcendentals=0),
        name='attend',
    )(cache_len, near(q_all), near(new_k_block), near(new_v_block), hidden, keep(w_o))
    return out_hidden, new_k_block, new_v_block


def solution(mesh):
    assert mesh.shape['sp'] == 2 * CHIPS
    cache_spec = P('dp', 'sp', None)
    return jax.shard_map(local_step, mesh=mesh, in_specs=(P('dp', None), P(None), P(None, None), P(None, None), P(None, None), P(None, None), cache_spec, cache_spec, P('dp')), out_specs=(P('dp', None), cache_spec, cache_spec), check_vma=False)
```

```python
import functools

import jax
import jax.numpy as jnp
from jax import lax
from jax.experimental import pallas as pl
from jax.experimental.pallas import tpu as pltpu
from jax.sharding import PartitionSpec as P

ROPE_BASE = 10000.0
EPSILON = 1e-6
MESH = pl.DeviceIdType.MESH
MIB = 1 << 20
LOWEST = float(jnp.finfo(jnp.float32).min)
CROWS = 8
CHIPS = 4


def rotate(x, cos_t, sin_t):
    half = x.shape[-1] // 2
    low, high = x[:, :half], x[:, half:]
    return jnp.concatenate([low * cos_t - high * sin_t, high * cos_t + low * sin_t], axis=-1)


def project_kernel(len_hbm, hid_hbm, wn_hbm, fr_ref, wk_hbm, wv_hbm, wq_hbm, q_ref, k_ref, v_ref, slot_ref,
                   lens, wn, hid, xn, wkv, wq, kv, mine, theirs, sem_l, sem_n, sem_h, sem_k, sem_v, sem_q, kv_s, kv_r,
                   x_s, x_r):
    f32, bf16 = jnp.float32, jnp.bfloat16
    rows = hid.shape[0]
    head_dim = wq.shape[2]
    heads, half = wq.shape[0], head_dim // 2
    brows = rows // q_ref.shape[1]
    me = lax.axis_index('sp')
    core = lax.rem(me, 2)
    partner = {'sp': me + 1 - 2 * core}

    def q_copy(j):
        columns = pl.ds(pl.multiple_of((core * heads + j) * head_dim, head_dim), head_dim)
        return pltpu.make_async_copy(wq_hbm.at[:, columns], wq.at[j], sem_q.at[j])

    def exchange(j):
        return pltpu.make_async_remote_copy(src_ref=mine.at[j], dst_ref=theirs.at[j], send_sem=x_s.at[j],
                                            recv_sem=x_r.at[j], device_id=partner, device_id_type=MESH)

    part = pl.ds(pl.multiple_of(core * half, half), half)
    l_copy = pltpu.make_async_copy(len_hbm, lens, sem_l)
    n_copy = pltpu.make_async_copy(wn_hbm, wn, sem_n)
    h_copy = pltpu.make_async_copy(hid_hbm, hid, sem_h)
    k_copy = pltpu.make_async_copy(wk_hbm.at[:, part], wkv.at[:, pl.ds(0, half)], sem_k)
    v_copy = pltpu.make_async_copy(wv_hbm.at[:, part], wkv.at[:, pl.ds(half, half)], sem_v)
    for copy in (l_copy, n_copy, h_copy, k_copy, v_copy):
        copy.start()
    for j in range(heads):
        q_copy(j).start()
    barrier = pltpu.get_barrier_semaphore()
    pl.semaphore_signal(barrier, inc=1, device_id=partner, device_id_type=MESH)

    l_copy.wait()
    lengths = lens[...].reshape(1, rows)
    across = lax.broadcasted_iota(jnp.int32, (rows, rows), 1)
    down = lax.broadcasted_iota(jnp.int32, (rows, rows), 0)
    column = jnp.sum(jnp.where(across == down, lengths, 0).astype(f32), axis=1, keepdims=True)
    slots = slot_ref.shape[1]
    slot = lax.broadcasted_iota(jnp.int32, (rows, slots), 1) + me * slots
    slot_ref[...] = (slot.astype(f32) == column).astype(jnp.int32)
    angles = column * fr_ref[...]
    cos_t, sin_t = jnp.cos(angles), jnp.sin(angles)

    n_copy.wait()
    gain = 1.0 + wn[...].astype(f32).reshape(1, wn.shape[0])
    h_copy.wait()
    x = hid[...].astype(f32)
    inv_rms = lax.rsqrt(jnp.mean(x * x, axis=-1, keepdims=True) + EPSILON)
    xn[...] = (x * inv_rms * gain).astype(bf16)

    def project(w):
        y = jnp.dot(xn[...], w, preferred_element_type=f32)
        return y.astype(bf16)

    k_copy.wait()
    v_copy.wait()
    y = project(wkv[...]).astype(f32)
    kv[core, 0] = y[:, 0:half]
    kv[core, 1] = y[:, half:2 * half]
    pl.semaphore_wait(barrier, 1)
    kv_copy = pltpu.make_async_remote_copy(src_ref=kv.at[core], dst_ref=kv.at[core], send_sem=kv_s, recv_sem=kv_r,
                                           device_id=partner, device_id_type=MESH)
    kv_copy.start()

    def place(k, j, y):
        for i in range(q_ref.shape[1]):
            for d in range(2):
                q_ref[k, i, d, pl.ds(j, brows, stride=heads), :] = y[i * brows:(i + 1) * brows, d * half:(d + 1) * half]

    def one_head(j, carry):
        q_copy(j).wait()
        y = project(wq[j]).astype(f32)
        mine[j] = (rotate(y, cos_t, sin_t) * head_dim ** -0.5).astype(bf16).astype(f32)
        exchange(j).start()
        place(core, j, mine[j])
        return carry

    lax.fori_loop(0, heads, one_head, 0)
    kv_copy.wait_recv()
    k_ref[...] = rotate(jnp.concatenate([kv[0, 0], kv[1, 0]], axis=-1), cos_t, sin_t).astype(bf16)
    v_ref[...] = jnp.concatenate([kv[0, 1], kv[1, 1]], axis=-1).astype(bf16)

    def their_head(j, carry):
        exchange(j).wait_recv()
        place(1 - core, j, theirs[j])
        return carry

    lax.fori_loop(0, heads, their_head, 0)
    kv_copy.wait_send()

    def finish(j, carry):
        exchange(j).wait_send()
        return carry

    lax.fori_loop(0, heads, finish, 0)


def attend_kernel(len_ref, q_all, kc_ref, vc_ref, hid_ref, wo_hbm, out_ref,
                  mine, theirs, r_recv, l_recv, from_left, from_right, att, a_bf, wo, gath, other,
                  sem_wo, d_s, d_r, rs_s, rs_r, at_s, at_r, own_s, own_r, fw_s, fw_r, h_s, h_r):
    f32, bf16 = jnp.float32, jnp.bfloat16
    me = lax.axis_index('sp')
    chip, core = me // 2, lax.rem(me, 2)
    mate = 1 - core
    peers = 2 * CHIPS
    slots = kc_ref.shape[1]
    urows = 2 * CROWS
    hrows = CROWS // 2
    hl = att.shape[4]
    heads = att.shape[3] // CROWS
    hh = heads // 2
    hd = 2 * hl
    nq = wo.shape[0]
    nm = own_s.shape[2]
    per = nq // nm
    data = mine.shape[4] - 8

    def at(c, k):
        return {'sp': lax.rem(c + CHIPS, CHIPS) * 2 + k}

    right, left = at(chip + 1, core), at(chip - 1, core)
    partner = at(chip, mate)

    def remote(src, dst, ssem, rsem, dev):
        return pltpu.make_async_remote_copy(src_ref=src, dst_ref=dst, send_sem=ssem, recv_sem=rsem,
                                            device_id=dev, device_id_type=MESH)

    def wo_copy(j):
        columns = pl.ds(pl.multiple_of((core * nq + j) * hd, hd), hd)
        return pltpu.make_async_copy(wo_hbm.at[:, columns], wo.at[j], sem_wo.at[j])

    for j in range(nq):
        wo_copy(j).start()

    barrier = pltpu.get_barrier_semaphore()
    for dev in (right, left, partner):
        pl.semaphore_signal(barrier, inc=1, device_id=dev, device_id_type=MESH)

    lane = lax.broadcasted_iota(jnp.int32, (heads, slots), 1)
    lane8 = lax.broadcasted_iota(jnp.int32, (8, 128), 1)
    is_max = lane8 < 64
    position = me * slots + lane

    def place_of(t):
        return lax.rem(chip + 2 - t + 3 * (t // 2) - 2 * (t // 3), CHIPS)

    def attention(ph, t):
        i = 2 * place_of(t) + ph
        for kk in range(2):
            for half in range(2):
                stat = jnp.zeros((8, 128), f32)
                for r4 in range(hrows):
                    r = kk * CROWS + half * hrows + r4
                    b = i * urows + r
                    own_rows = slice(r * hh, (r + 1) * hh)
                    q = jnp.concatenate([
                        jnp.concatenate([q_all[k, i, d, own_rows, :] for k in range(2)], axis=0) for d in range(2)], axis=1)
                    s = lax.dot_general(q.astype(bf16), kc_ref[b], (((1,), (1,)), ((), ())), preferred_element_type=f32)
                    valid = position <= len_ref[b]
                    s = jnp.where(valid, s, LOWEST)
                    m = jnp.max(s, axis=1, keepdims=True)
                    p = jnp.where(valid, jnp.exp(s - m), 0.0)
                    den = jnp.sum(p, axis=1, keepdims=True)
                    o = jnp.dot(p.astype(bf16), vc_ref[b], preferred_element_type=f32)
                    for d in range(2):
                        rows = slice((d * hrows + r4) * heads, (d * hrows + r4 + 1) * heads)
                        mine[ph, t, kk, half, rows, :] = o[:, d * hl:(d + 1) * hl]
                    for g in range(2):
                        stat = jnp.where(lane8 == g * 32 + r4, m[g * 8:(g + 1) * 8],
                                         jnp.where(lane8 == 64 + g * 32 + r4, den[g * 8:(g + 1) * 8], stat))
                mine[ph, t, kk, half, data:data + 8, :] = stat

    def d_copy(ph, t):
        return remote(mine.at[ph, t, mate], theirs.at[ph, t], d_s.at[ph, t], d_r.at[ph, t], partner)

    def tiles():
        for r4 in range(hrows):
            for g in range(2):
                for d in range(2):
                    yield g * 32 + r4, (d * hrows + r4) * heads + g * 8, d, r4, g

    def merge(into, src):
        one, two = into[data:data + 8, :], src[data:data + 8, :]
        top = jnp.maximum(one, two)
        a, b = jnp.exp(one - top), jnp.exp(two - top)
        den = pltpu.roll(a, 64, 1) * one + pltpu.roll(b, 64, 1) * two
        for column, row, _, _, _ in tiles():
            into[row:row + 8, :] = (into[row:row + 8, :] * a[:, column:column + 1]
                                    + src[row:row + 8, :] * b[:, column:column + 1])
        into[data:data + 8, :] = jnp.where(is_max, top, den)

    def combine(ph, t):
        d_copy(ph, t).wait_recv()
        for half in range(2):
            merge(mine.at[ph, t, core, half], theirs.at[ph, t, half])

    def ring(ph, n, src, dst, dev):
        return remote(src, dst, rs_s.at[ph, n], rs_r.at[ph, n], dev)

    def piece(ph, t, half):
        return mine.at[ph, t, core, half]

    def r1(ph):
        return ring(ph, 0, piece(ph, 0, 0), r_recv.at[ph], right)

    def l1(ph):
        return ring(ph, 1, piece(ph, 0, 1), l_recv.at[ph], left)

    def r2(ph, half):
        return ring(ph, 2 + half, piece(ph, 1, half), from_left.at[ph, half], right)

    def l2(ph, half):
        return ring(ph, 4 + half, piece(ph, 2, half), from_right.at[ph, half], left)

    def reduce_start(ph):
        combine(ph, 0)
        r1(ph).start()
        l1(ph).start()
        combine(ph, 1)
        r2(ph, 1).start()
        combine(ph, 2)
        l2(ph, 0).start()

    def reduce_turn(ph):
        r1(ph).wait_recv()
        merge(piece(ph, 1, 0), r_recv.at[ph])
        r2(ph, 0).start()
        l1(ph).wait_recv()
        merge(piece(ph, 2, 1), l_recv.at[ph])
        l2(ph, 1).start()

    def at_copy(ph):
        return remote(att.at[ph, core], att.at[ph, core], at_s.at[ph], at_r.at[ph], partner)

    def reduce_end(ph):
        for half in range(2):
            r2(ph, half).wait_recv()
            l2(ph, half).wait_recv()
            parts = [mine.at[ph, 3, core, half], from_left.at[ph, half], from_right.at[ph, half]]
            stats = [x[data:data + 8, :] for x in parts]
            top = jnp.maximum(jnp.maximum(stats[0], stats[1]), stats[2])
            scale = [jnp.exp(x - top) for x in stats]
            den = sum(a * pltpu.roll(x, 64, 1) for a, x in zip(scale, stats))
            den = jnp.where(is_max & (lane8 % 32 < hrows), den, 1.0)
            scale = [a / den for a in scale]
            for column, row, d, r4, g in tiles():
                y = sum(x[row:row + 8, :] * a[:, column:column + 1] for x, a in zip(parts, scale))
                to = (half * hrows + r4) * heads + g * 8
                att[ph, core, d, to:to + 8, :] = y
        at_copy(ph).start()

    def rows_of(c, ph):
        return pl.ds(pl.multiple_of((2 * c + ph) * urows, urows), urows)

    def columns_of(k, n):
        return pl.ds(pl.multiple_of((k * nq + n) * hd, hd), hd)

    def own_copies(ph, u):
        src = gath.at[ph, chip, pl.ds(u * per, per)]
        return (remote(src, src, own_s.at[ph, 0, u], own_r.at[ph, 0, u], right),
                remote(src, src, own_s.at[ph, 1, u], own_r.at[ph, 1, u], left),
                to_mate(ph, 0, chip, u))

    def to_mate(ph, which, c, u):
        part = pl.ds(u * per, per)
        return remote(gath.at[ph, c, part], other.at[ph, c, part], h_s.at[ph, which, u], h_r.at[ph, which, u], partner)

    def project(ph, first):
        at_copy(ph).wait_recv()
        for h in range(heads):
            for d in range(2):
                pair = [att[ph, kk, d, pl.ds(h, CROWS, stride=heads), :] for kk in range(2)]
                a_bf[ph, :, h * hd + d * hl:h * hd + (d + 1) * hl] = jnp.concatenate(pair, axis=0).astype(bf16)

        def message(u, carry):
            for v in range(per):
                n = u * per + v
                if first:
                    wo_copy(n).wait()
                y = jnp.dot(a_bf[ph], wo[n], preferred_element_type=f32)
                gath[ph, chip, n] = hid_ref[rows_of(chip, ph), columns_of(core, n)].astype(f32) + y
            for copy in own_copies(ph, u):
                copy.start()
            return carry

        lax.fori_loop(0, nm, message, 0)

    cl, cr, co = place_of(2), place_of(1), place_of(0)
    split = nm // 2

    def forward(ph, u):
        c, dev = (cl, right) if u < split else (cr, left)
        src = gath.at[ph, c, pl.ds(u * per, per)]
        return remote(src, src, fw_s.at[ph, u], fw_r.at[ph, u], dev)

    def put(ph, c, u):
        for n in range(u * per, (u + 1) * per):
            out_ref[rows_of(c, ph), columns_of(core, n)] = gath[ph, c, n].astype(bf16)

    def put_other(ph, c, u):
        for n in range(u * per, (u + 1) * per):
            out_ref[rows_of(c, ph), columns_of(mate, n)] = other[ph, c, n].astype(bf16)

    def relay(ph):
        for u in range(nm):
            own_copies(ph, u)[0].wait_recv()
            if u < split:
                forward(ph, u).start()
            to_mate(ph, 1, cl, u).start()
            own_copies(ph, u)[1].wait_recv()
            if u >= split:
                forward(ph, u).start()
            to_mate(ph, 2, cr, u).start()

    def relay_end(ph):
        for u in range(nm):
            forward(ph, u).wait_recv()
            to_mate(ph, 3, co, u).start()

    places = ((0, chip), (1, cl), (2, cr), (3, co))

    def finish(ph):
        for which, c in places:
            for u in range(nm):
                put(ph, c, u)
                to_mate(ph, which, c, u).wait_recv()
                put_other(ph, c, u)

    def unit(ph):
        def body(t, carry):
            attention(ph, t)
            d_copy(ph, t).start()
            return carry

        return body

    attention(0, 0)
    pl.semaphore_wait(barrier, 3)
    d_copy(0, 0).start()
    lax.fori_loop(1, CHIPS, unit(0), 0)
    reduce_start(0)
    lax.fori_loop(0, CHIPS, unit(1), 0)
    reduce_turn(0)
    reduce_start(1)
    combine(0, 3)
    reduce_turn(1)
    combine(1, 3)
    reduce_end(0)
    project(0, True)
    reduce_end(1)
    project(1, False)
    relay(0)
    relay_end(0)
    relay(1)
    finish(0)
    relay_end(1)
    finish(1)

    for ph in range(2):
        for t in range(CHIPS):
            d_copy(ph, t).wait_send()
        for copy in (r1(ph), l1(ph), r2(ph, 0), r2(ph, 1), l2(ph, 0), l2(ph, 1), at_copy(ph)):
            copy.wait_send()
        for u in range(nm):
            for copy in own_copies(ph, u):
                copy.wait_send()
            forward(ph, u).wait_send()
            for which, c in places[1:]:
                to_mate(ph, which, c, u).wait_send()


def local_step(hidden, w_norm, w_q, w_k, w_v, w_o, k_block, v_block, cache_len):
    f32, bf16 = jnp.float32, jnp.bfloat16
    rows, width = hidden.shape
    seq_block, hd = k_block.shape[1], k_block.shape[2]
    heads = w_q.shape[1] // hd
    hh, hl = heads // 2, hd // 2
    nblk = 2 * CHIPS
    brows = rows // nblk
    assert brows == 2 * CROWS
    inv_freq = (ROPE_BASE ** (-jnp.arange(hl, dtype=f32) * 2.0 / hd)).reshape(1, hl)
    vmem = pl.BlockSpec(memory_space=pltpu.VMEM)
    hbm = pl.BlockSpec(memory_space=pl.ANY)
    smem = pl.BlockSpec(memory_space=pltpu.SMEM)
    dma = pltpu.SemaphoreType.DMA

    def keep(x):
        return pltpu.with_memory_space_constraint(x, pltpu.HBM)

    def near(x):
        return pltpu.with_memory_space_constraint(x, pltpu.VMEM)

    q_all, k_rot, v_new, slot = pl.pallas_call(
        project_kernel,
        out_shape=(pltpu.VMEM((2, nblk, 2, brows * hh, hl), f32), jax.ShapeDtypeStruct((rows, hd), bf16),
                   jax.ShapeDtypeStruct((rows, hd), bf16), jax.ShapeDtypeStruct((rows, seq_block), jnp.int32)),
        in_specs=[hbm] * 3 + [vmem] + [hbm] * 3,
        out_specs=(vmem,) * 4,
        scratch_shapes=[
            pltpu.VMEM((rows,), jnp.int32),
            pltpu.VMEM((width,), bf16),
            pltpu.VMEM((rows, width), bf16),
            pltpu.VMEM((rows, width), bf16),
            pltpu.VMEM((width, hd), bf16),
            pltpu.VMEM((hh, width, hd), bf16),
            pltpu.VMEM((2, 2, rows, hl), f32),
            pltpu.VMEM((hh, rows, hd), f32),
            pltpu.VMEM((hh, rows, hd), f32),
            dma, dma, dma, dma, dma, dma((hh,)), dma, dma, dma((hh,)), dma((hh,)),
        ],
        compiler_params=pltpu.CompilerParams(collective_id=1, has_side_effects=True, vmem_limit_bytes=56 * MIB),
        cost_estimate=pl.CostEstimate(flops=2 * rows * width * (hh + 1) * hd, bytes_accessed=2 * width * (hh + 1) * hd,
                                      transcendentals=0),
        name='project',
    )(keep(cache_len), keep(hidden), keep(w_norm), inv_freq, keep(w_k), keep(w_v), keep(w_q))

    at_slot = (slot != 0)[:, :, None]
    new_k_block = jnp.where(at_slot, k_rot[:, None, :], k_block)
    new_v_block = jnp.where(at_slot, v_new[:, None, :], v_block)

    half_rows = CROWS * heads + 8
    nm = hh // 2
    out_hidden = pl.pallas_call(
        attend_kernel,
        out_shape=jax.ShapeDtypeStruct((rows, width), bf16),
        in_specs=[smem, vmem, vmem, vmem, vmem, hbm],
        out_specs=vmem,
        scratch_shapes=[
            pltpu.VMEM((2, CHIPS, 2, 2, half_rows, hl), f32),
            pltpu.VMEM((2, CHIPS, 2, half_rows, hl), f32),
            pltpu.VMEM((2, half_rows, hl), f32),
            pltpu.VMEM((2, half_rows, hl), f32),
            pltpu.VMEM((2, 2, half_rows, hl), f32),
            pltpu.VMEM((2, 2, half_rows, hl), f32),
            pltpu.VMEM((2, 2, 2, CROWS * heads, hl), f32),
            pltpu.VMEM((2, brows, width), bf16),
            pltpu.VMEM((hh, width, hd), bf16),
            pltpu.VMEM((2, CHIPS, hh, brows, hd), f32),
            pltpu.VMEM((2, CHIPS, hh, brows, hd), f32),
            dma((hh,)), dma((2, CHIPS)), dma((2, CHIPS)), dma((2, 6)), dma((2, 6)), dma((2,)), dma((2,)),
            dma((2, 2, nm)), dma((2, 2, nm)), dma((2, nm)), dma((2, nm)), dma((2, CHIPS, nm)), dma((2, CHIPS, nm)),
        ],
        compiler_params=pltpu.CompilerParams(collective_id=0, has_side_effects=True, vmem_limit_bytes=26 * MIB),
        cost_estimate=pl.CostEstimate(flops=2 * rows * width * hh * hd * 2, bytes_accessed=2 * width * hh * hd,
                                      transcendentals=0),
        name='attend',
    )(cache_len, near(q_all), near(new_k_block), near(new_v_block), hidden, keep(w_o))
    return out_hidden, new_k_block, new_v_block


def solution(mesh):
    assert mesh.shape['sp'] == 2 * CHIPS
    cache_spec = P('dp', 'sp', None)
    return jax.shard_map(local_step, mesh=mesh, in_specs=(P('dp', None), P(None), P(None, None), P(None, None), P(None, None), P(None, None), cache_spec, cache_spec, P('dp')), out_specs=(P('dp', None), cache_spec, cache_spec), check_vma=False)
```

```python
import functools

import jax
import jax.numpy as jnp
from jax import lax
from jax.experimental import pallas as pl
from jax.experimental.pallas import tpu as pltpu
from jax.sharding import PartitionSpec as P

ROPE_BASE = 10000.0
EPSILON = 1e-6
MESH = pl.DeviceIdType.MESH
MIB = 1 << 20
LOWEST = float(jnp.finfo(jnp.float32).min)
CROWS = 8
CHIPS = 4


def rotate(x, cos_t, sin_t):
    half = x.shape[-1] // 2
    low, high = x[:, :half], x[:, half:]
    return jnp.concatenate([low * cos_t - high * sin_t, high * cos_t + low * sin_t], axis=-1)


def project_kernel(slots, len_hbm, hid_hbm, wn_hbm, fr_ref, wk_hbm, wv_hbm, wq_hbm, q_ref, k_ref, v_ref, slot_ref,
                   lens, wn, hid, xn, wkv, wq, kv, mine, theirs, sem_l, sem_n, sem_h, sem_k, sem_v, sem_q, kv_s, kv_r,
                   x_s, x_r):
    f32, bf16 = jnp.float32, jnp.bfloat16
    rows = hid.shape[0]
    head_dim = wq.shape[2]
    heads, half = wq.shape[0], head_dim // 2
    brows = rows // q_ref.shape[1]
    me = lax.axis_index('sp')
    core = lax.rem(me, 2)
    partner = {'sp': me + 1 - 2 * core}

    def q_copy(j):
        columns = pl.ds(pl.multiple_of((core * heads + j) * head_dim, head_dim), head_dim)
        return pltpu.make_async_copy(wq_hbm.at[:, columns], wq.at[j], sem_q.at[j])

    def exchange(j):
        return pltpu.make_async_remote_copy(src_ref=mine.at[j], dst_ref=theirs.at[j], send_sem=x_s.at[j],
                                            recv_sem=x_r.at[j], device_id=partner, device_id_type=MESH)

    part = pl.ds(pl.multiple_of(core * half, half), half)
    l_copy = pltpu.make_async_copy(len_hbm, lens, sem_l)
    n_copy = pltpu.make_async_copy(wn_hbm, wn, sem_n)
    h_copy = pltpu.make_async_copy(hid_hbm, hid, sem_h)
    k_copy = pltpu.make_async_copy(wk_hbm.at[:, part], wkv.at[:, pl.ds(0, half)], sem_k)
    v_copy = pltpu.make_async_copy(wv_hbm.at[:, part], wkv.at[:, pl.ds(half, half)], sem_v)
    for copy in (l_copy, n_copy, h_copy, k_copy, v_copy):
        copy.start()
    ahead = 3
    for j in range(ahead):
        q_copy(j).start()
    barrier = pltpu.get_barrier_semaphore()
    pl.semaphore_signal(barrier, inc=1, device_id=partner, device_id_type=MESH)

    l_copy.wait()
    lengths = lens[...].reshape(1, rows)
    across = lax.broadcasted_iota(jnp.int32, (rows, rows), 1)
    down = lax.broadcasted_iota(jnp.int32, (rows, rows), 0)
    column = jnp.sum(jnp.where(across == down, lengths, 0).astype(f32), axis=1, keepdims=True)
    first = (me * slots).astype(f32)
    slot_ref[...] = jnp.broadcast_to((column - first).astype(jnp.int32), slot_ref.shape)
    angles = column * fr_ref[...]
    cos_t, sin_t = jnp.cos(angles), jnp.sin(angles)

    n_copy.wait()
    gain = 1.0 + wn[...].astype(f32).reshape(1, wn.shape[0])
    h_copy.wait()
    x = hid[...].astype(f32)
    inv_rms = lax.rsqrt(jnp.mean(x * x, axis=-1, keepdims=True) + EPSILON)
    xn[...] = (x * inv_rms * gain).astype(bf16)

    def project(w):
        y = jnp.dot(xn[...], w, preferred_element_type=f32)
        return y.astype(bf16)

    k_copy.wait()
    v_copy.wait()
    y = project(wkv[...]).astype(f32)
    kv[core, 0] = y[:, 0:half]
    kv[core, 1] = y[:, half:2 * half]
    pl.semaphore_wait(barrier, 1)
    kv_copy = pltpu.make_async_remote_copy(src_ref=kv.at[core], dst_ref=kv.at[core], send_sem=kv_s, recv_sem=kv_r,
                                           device_id=partner, device_id_type=MESH)
    kv_copy.start()

    def place(k, j, y):
        for i in range(q_ref.shape[1]):
            for d in range(2):
                q_ref[k, i, d, pl.ds(j, brows, stride=heads), :] = y[i * brows:(i + 1) * brows, d * half:(d + 1) * half]

    def one_head(j, carry):
        q_copy(j).wait()

        @pl.when(j + ahead < heads)
        def _():
            q_copy(j + ahead).start()

        y = project(wq[j]).astype(f32)
        mine[j] = (rotate(y, cos_t, sin_t) * head_dim ** -0.5).astype(bf16).astype(f32)
        exchange(j).start()
        place(core, j, mine[j])
        return carry

    lax.fori_loop(0, heads, one_head, 0)
    kv_copy.wait_recv()
    k_ref[...] = rotate(jnp.concatenate([kv[0, 0], kv[1, 0]], axis=-1), cos_t, sin_t).astype(bf16)
    v_ref[...] = jnp.concatenate([kv[0, 1], kv[1, 1]], axis=-1).astype(bf16)

    def their_head(j, carry):
        exchange(j).wait_recv()
        place(1 - core, j, theirs[j])
        return carry

    lax.fori_loop(0, heads, their_head, 0)
    kv_copy.wait_send()

    def finish(j, carry):
        exchange(j).wait_send()
        return carry

    lax.fori_loop(0, heads, finish, 0)


def attend_kernel(len_ref, q_all, kc_ref, vc_ref, hid_ref, wo_hbm, out_ref,
                  p_buf, mine, theirs, r_recv, l_recv, from_left, from_right, att, a_bf, wo, gath, other,
                  sem_wo, d_s, d_r, rs_s, rs_r, at_s, at_r, own_s, own_r, fw_s, fw_r, h_s, h_r):
    f32, bf16 = jnp.float32, jnp.bfloat16
    me = lax.axis_index('sp')
    chip, core = me // 2, lax.rem(me, 2)
    mate = 1 - core
    peers = 2 * CHIPS
    slots = kc_ref.shape[1]
    urows = 2 * CROWS
    hrows = CROWS // 2
    hl = att.shape[4]
    heads = att.shape[3] // CROWS
    hh = heads // 2
    hd = 2 * hl
    nq = wo.shape[0]
    nm = own_s.shape[2]
    per = nq // nm
    data = mine.shape[4] - 8

    def at(c, k):
        return {'sp': lax.rem(c + CHIPS, CHIPS) * 2 + k}

    right, left = at(chip + 1, core), at(chip - 1, core)
    partner = at(chip, mate)

    def remote(src, dst, ssem, rsem, dev):
        return pltpu.make_async_remote_copy(src_ref=src, dst_ref=dst, send_sem=ssem, recv_sem=rsem,
                                            device_id=dev, device_id_type=MESH)

    def wo_copy(j):
        columns = pl.ds(pl.multiple_of((core * nq + j) * hd, hd), hd)
        return pltpu.make_async_copy(wo_hbm.at[:, columns], wo.at[j], sem_wo.at[j])

    for j in range(nq):
        wo_copy(j).start()

    barrier = pltpu.get_barrier_semaphore()
    for dev in (right, left, partner):
        pl.semaphore_signal(barrier, inc=1, device_id=dev, device_id_type=MESH)

    lane = lax.broadcasted_iota(jnp.int32, (heads, slots), 1)
    lane8 = lax.broadcasted_iota(jnp.int32, (8, 128), 1)
    is_max = lane8 < 64
    position = me * slots + lane

    def place_of(t):
        return lax.rem(chip + 2 - t + 3 * (t // 2) - 2 * (t // 3), CHIPS)

    def scores(ph, t):
        i = 2 * place_of(t) + ph
        for kk in range(2):
            for half in range(2):
                stat = jnp.zeros((8, 128), f32)
                for r4 in range(hrows):
                    r = kk * CROWS + half * hrows + r4
                    b = i * urows + r
                    own_rows = slice(r * hh, (r + 1) * hh)
                    q = jnp.concatenate([
                        jnp.concatenate([q_all[k, i, d, own_rows, :] for k in range(2)], axis=0) for d in range(2)], axis=1)
                    s = lax.dot_general(q.astype(bf16), kc_ref[b], (((1,), (1,)), ((), ())), preferred_element_type=f32)
                    valid = position <= len_ref[b]
                    s = jnp.where(valid, s, LOWEST)
                    m = jnp.max(s, axis=1, keepdims=True)
                    p = jnp.where(valid, jnp.exp(s - m), 0.0)
                    den = jnp.sum(p, axis=1, keepdims=True)
                    p_buf[t, r] = p.astype(bf16)
                    for g in range(2):
                        stat = jnp.where(lane8 == g * 32 + r4, m[g * 8:(g + 1) * 8],
                                         jnp.where(lane8 == 64 + g * 32 + r4, den[g * 8:(g + 1) * 8], stat))
                mine[ph, t, kk, half, data:data + 8, :] = stat

    def values(ph, t):
        i = 2 * place_of(t) + ph
        for kk in range(2):
            for half in range(2):
                for r4 in range(hrows):
                    r = kk * CROWS + half * hrows + r4
                    o = jnp.dot(p_buf[t, r], vc_ref[i * urows + r], preferred_element_type=f32)
                    for d in range(2):
                        rows = slice((d * hrows + r4) * heads, (d * hrows + r4 + 1) * heads)
                        mine[ph, t, kk, half, rows, :] = o[:, d * hl:(d + 1) * hl]

    def d_copy(ph, t):
        return remote(mine.at[ph, t, mate], theirs.at[ph, t], d_s.at[ph, t], d_r.at[ph, t], partner)

    def tiles():
        for r4 in range(hrows):
            for g in range(2):
                for d in range(2):
                    yield g * 32 + r4, (d * hrows + r4) * heads + g * 8, d, r4, g

    def merge(into, src):
        one, two = into[data:data + 8, :], src[data:data + 8, :]
        top = jnp.maximum(one, two)
        a, b = jnp.exp(one - top), jnp.exp(two - top)
        den = pltpu.roll(a, 64, 1) * one + pltpu.roll(b, 64, 1) * two
        for column, row, _, _, _ in tiles():
            into[row:row + 8, :] = (into[row:row + 8, :] * a[:, column:column + 1]
                                    + src[row:row + 8, :] * b[:, column:column + 1])
        into[data:data + 8, :] = jnp.where(is_max, top, den)

    def combine(ph, t):
        d_copy(ph, t).wait_recv()
        for half in range(2):
            merge(mine.at[ph, t, core, half], theirs.at[ph, t, half])

    def ring(ph, n, src, dst, dev):
        return remote(src, dst, rs_s.at[ph, n], rs_r.at[ph, n], dev)

    def piece(ph, t, half):
        return mine.at[ph, t, core, half]

    def r1(ph):
        return ring(ph, 0, piece(ph, 0, 0), r_recv.at[ph], right)

    def l1(ph):
        return ring(ph, 1, piece(ph, 0, 1), l_recv.at[ph], left)

    def r2(ph, half):
        return ring(ph, 2 + half, piece(ph, 1, half), from_left.at[ph, half], right)

    def l2(ph, half):
        return ring(ph, 4 + half, piece(ph, 2, half), from_right.at[ph, half], left)

    def reduce_start(ph):
        combine(ph, 0)
        r1(ph).start()
        l1(ph).start()
        combine(ph, 1)
        r2(ph, 1).start()
        combine(ph, 2)
        l2(ph, 0).start()

    def reduce_turn(ph):
        r1(ph).wait_recv()
        merge(piece(ph, 1, 0), r_recv.at[ph])
        r2(ph, 0).start()
        l1(ph).wait_recv()
        merge(piece(ph, 2, 1), l_recv.at[ph])
        l2(ph, 1).start()

    def at_copy(ph):
        return remote(att.at[ph, core], att.at[ph, core], at_s.at[ph], at_r.at[ph], partner)

    def reduce_end(ph):
        for half in range(2):
            r2(ph, half).wait_recv()
            l2(ph, half).wait_recv()
            parts = [mine.at[ph, 3, core, half], from_left.at[ph, half], from_right.at[ph, half]]
            stats = [x[data:data + 8, :] for x in parts]
            top = jnp.maximum(jnp.maximum(stats[0], stats[1]), stats[2])
            scale = [jnp.exp(x - top) for x in stats]
            den = sum(a * pltpu.roll(x, 64, 1) for a, x in zip(scale, stats))
            den = jnp.where(is_max & (lane8 % 32 < hrows), den, 1.0)
            scale = [a / den for a in scale]
            for column, row, d, r4, g in tiles():
                y = sum(x[row:row + 8, :] * a[:, column:column + 1] for x, a in zip(parts, scale))
                to = (half * hrows + r4) * heads + g * 8
                att[ph, core, d, to:to + 8, :] = y
        at_copy(ph).start()

    def rows_of(c, ph):
        return pl.ds(pl.multiple_of((2 * c + ph) * urows, urows), urows)

    def columns_of(k, n):
        return pl.ds(pl.multiple_of((k * nq + n) * hd, hd), hd)

    def own_copies(ph, u):
        src = gath.at[ph, chip, pl.ds(u * per, per)]
        return (remote(src, src, own_s.at[ph, 0, u], own_r.at[ph, 0, u], right),
                remote(src, src, own_s.at[ph, 1, u], own_r.at[ph, 1, u], left),
                to_mate(ph, 0, chip, u))

    def to_mate(ph, which, c, u):
        part = pl.ds(u * per, per)
        return remote(gath.at[ph, c, part], other.at[ph, c, part], h_s.at[ph, which, u], h_r.at[ph, which, u], partner)

    def project(ph, first):
        at_copy(ph).wait_recv()
        for h in range(heads):
            for d in range(2):
                pair = [att[ph, kk, d, pl.ds(h, CROWS, stride=heads), :] for kk in range(2)]
                a_bf[ph, :, h * hd + d * hl:h * hd + (d + 1) * hl] = jnp.concatenate(pair, axis=0).astype(bf16)

        def message(u, carry):
            for v in range(per):
                n = u * per + v
                if first:
                    wo_copy(n).wait()
                y = jnp.dot(a_bf[ph], wo[n], preferred_element_type=f32)
                gath[ph, chip, n] = hid_ref[rows_of(chip, ph), columns_of(core, n)].astype(f32) + y
            for copy in own_copies(ph, u):
                copy.start()
            return carry

        lax.fori_loop(0, nm, message, 0)

    cl, cr, co = place_of(2), place_of(1), place_of(0)
    split = nm // 2

    def forward(ph, u):
        c, dev = (cl, right) if u < split else (cr, left)
        src = gath.at[ph, c, pl.ds(u * per, per)]
        return remote(src, src, fw_s.at[ph, u], fw_r.at[ph, u], dev)

    def put(ph, c, u):
        for n in range(u * per, (u + 1) * per):
            out_ref[rows_of(c, ph), columns_of(core, n)] = gath[ph, c, n].astype(bf16)

    def put_other(ph, c, u):
        for n in range(u * per, (u + 1) * per):
            out_ref[rows_of(c, ph), columns_of(mate, n)] = other[ph, c, n].astype(bf16)

    def relay(ph):
        for u in range(nm):
            own_copies(ph, u)[0].wait_recv()
            if u < split:
                forward(ph, u).start()
            to_mate(ph, 1, cl, u).start()
            own_copies(ph, u)[1].wait_recv()
            if u >= split:
                forward(ph, u).start()
            to_mate(ph, 2, cr, u).start()

    def relay_end(ph):
        for u in range(nm):
            forward(ph, u).wait_recv()
            to_mate(ph, 3, co, u).start()

    places = ((0, chip), (1, cl), (2, cr), (3, co))

    def finish(ph):
        for which, c in places:
            for u in range(nm):
                put(ph, c, u)
                to_mate(ph, which, c, u).wait_recv()
                put_other(ph, c, u)

    def scores_of(ph):
        def body(t, carry):
            scores(ph, t)
            return carry

        lax.fori_loop(0, CHIPS, body, 0)

    def values_of(ph):
        def body(t, carry):
            values(ph, t)
            d_copy(ph, t).start()
            return carry

        lax.fori_loop(0, CHIPS, body, 0)

    scores_of(0)
    pl.semaphore_wait(barrier, 3)
    values_of(0)
    scores_of(1)
    reduce_start(0)
    values_of(1)
    reduce_turn(0)
    reduce_start(1)
    combine(0, 3)
    reduce_turn(1)
    combine(1, 3)
    reduce_end(0)
    project(0, True)
    reduce_end(1)
    project(1, False)
    relay(0)
    relay_end(0)
    relay(1)
    finish(0)
    relay_end(1)
    finish(1)

    for ph in range(2):
        for t in range(CHIPS):
            d_copy(ph, t).wait_send()
        for copy in (r1(ph), l1(ph), r2(ph, 0), r2(ph, 1), l2(ph, 0), l2(ph, 1), at_copy(ph)):
            copy.wait_send()
        for u in range(nm):
            for copy in own_copies(ph, u):
                copy.wait_send()
            forward(ph, u).wait_send()
            for which, c in places[1:]:
                to_mate(ph, which, c, u).wait_send()


def local_step(hidden, w_norm, w_q, w_k, w_v, w_o, k_block, v_block, cache_len):
    f32, bf16 = jnp.float32, jnp.bfloat16
    rows, width = hidden.shape
    seq_block, hd = k_block.shape[1], k_block.shape[2]
    heads = w_q.shape[1] // hd
    hh, hl = heads // 2, hd // 2
    nblk = 2 * CHIPS
    brows = rows // nblk
    assert brows == 2 * CROWS
    inv_freq = (ROPE_BASE ** (-jnp.arange(hl, dtype=f32) * 2.0 / hd)).reshape(1, hl)
    vmem = pl.BlockSpec(memory_space=pltpu.VMEM)
    hbm = pl.BlockSpec(memory_space=pl.ANY)
    smem = pl.BlockSpec(memory_space=pltpu.SMEM)
    dma = pltpu.SemaphoreType.DMA

    def keep(x):
        return pltpu.with_memory_space_constraint(x, pltpu.HBM)

    def near(x):
        return pltpu.with_memory_space_constraint(x, pltpu.VMEM)

    q_all, k_rot, v_new, slot = pl.pallas_call(
        functools.partial(project_kernel, seq_block),
        out_shape=(pltpu.VMEM((2, nblk, 2, brows * hh, hl), f32), jax.ShapeDtypeStruct((rows, hd), bf16),
                   jax.ShapeDtypeStruct((rows, hd), bf16), jax.ShapeDtypeStruct((rows, hd), jnp.int32)),
        in_specs=[hbm] * 3 + [vmem] + [hbm] * 3,
        out_specs=(vmem,) * 4,
        scratch_shapes=[
            pltpu.VMEM((rows,), jnp.int32),
            pltpu.VMEM((width,), bf16),
            pltpu.VMEM((rows, width), bf16),
            pltpu.VMEM((rows, width), bf16),
            pltpu.VMEM((width, hd), bf16),
            pltpu.VMEM((hh, width, hd), bf16),
            pltpu.VMEM((2, 2, rows, hl), f32),
            pltpu.VMEM((hh, rows, hd), f32),
            pltpu.VMEM((hh, rows, hd), f32),
            dma, dma, dma, dma, dma, dma((hh,)), dma, dma, dma((hh,)), dma((hh,)),
        ],
        compiler_params=pltpu.CompilerParams(collective_id=1, has_side_effects=True, vmem_limit_bytes=56 * MIB),
        cost_estimate=pl.CostEstimate(flops=2 * rows * width * (hh + 1) * hd, bytes_accessed=2 * width * (hh + 1) * hd,
                                      transcendentals=0),
        name='project',
    )(keep(cache_len), keep(hidden), keep(w_norm), inv_freq, keep(w_k), keep(w_v), keep(w_q))

    at_slot = lax.broadcasted_iota(jnp.int32, k_block.shape, 1) == slot[:, None, :]
    new_k_block = jnp.where(at_slot, k_rot[:, None, :], k_block)
    new_v_block = jnp.where(at_slot, v_new[:, None, :], v_block)

    half_rows = CROWS * heads + 8
    nm = hh // 2
    out_hidden = pl.pallas_call(
        attend_kernel,
        out_shape=jax.ShapeDtypeStruct((rows, width), bf16),
        in_specs=[smem, vmem, vmem, vmem, vmem, hbm],
        out_specs=vmem,
        scratch_shapes=[
            pltpu.VMEM((CHIPS, brows, heads, seq_block), bf16),
            pltpu.VMEM((2, CHIPS, 2, 2, half_rows, hl), f32),
            pltpu.VMEM((2, CHIPS, 2, half_rows, hl), f32),
            pltpu.VMEM((2, half_rows, hl), f32),
            pltpu.VMEM((2, half_rows, hl), f32),
            pltpu.VMEM((2, 2, half_rows, hl), f32),
            pltpu.VMEM((2, 2, half_rows, hl), f32),
            pltpu.VMEM((2, 2, 2, CROWS * heads, hl), f32),
            pltpu.VMEM((2, brows, width), bf16),
            pltpu.VMEM((hh, width, hd), bf16),
            pltpu.VMEM((2, CHIPS, hh, brows, hd), f32),
            pltpu.VMEM((2, CHIPS, hh, brows, hd), f32),
            dma((hh,)), dma((2, CHIPS)), dma((2, CHIPS)), dma((2, 6)), dma((2, 6)), dma((2,)), dma((2,)),
            dma((2, 2, nm)), dma((2, 2, nm)), dma((2, nm)), dma((2, nm)), dma((2, CHIPS, nm)), dma((2, CHIPS, nm)),
        ],
        compiler_params=pltpu.CompilerParams(collective_id=0, has_side_effects=True, vmem_limit_bytes=26 * MIB),
        cost_estimate=pl.CostEstimate(flops=2 * rows * width * hh * hd * 2, bytes_accessed=2 * width * hh * hd,
                                      transcendentals=0),
        name='attend',
    )(cache_len, near(q_all), near(new_k_block), near(new_v_block), hidden, keep(w_o))
    return out_hidden, new_k_block, new_v_block


def solution(mesh):
    assert mesh.shape['sp'] == 2 * CHIPS
    cache_spec = P('dp', 'sp', None)
    return jax.shard_map(local_step, mesh=mesh, in_specs=(P('dp', None), P(None), P(None, None), P(None, None), P(None, None), P(None, None), cache_spec, cache_spec, P('dp')), out_specs=(P('dp', None), cache_spec, cache_spec), check_vma=False)
```

```python
import functools

import jax
import jax.numpy as jnp
from jax import lax
from jax.experimental import pallas as pl
from jax.experimental.pallas import tpu as pltpu
from jax.sharding import PartitionSpec as P

ROPE_BASE = 10000.0
EPSILON = 1e-6
MESH = pl.DeviceIdType.MESH
MIB = 1 << 20
LOWEST = float(jnp.finfo(jnp.float32).min)
CROWS = 8
CHIPS = 4


def rotate(x, cos_t, sin_t):
    half = x.shape[-1] // 2
    low, high = x[:, :half], x[:, half:]
    return jnp.concatenate([low * cos_t - high * sin_t, high * cos_t + low * sin_t], axis=-1)


def project_kernel(slots, len_hbm, hid_hbm, wn_hbm, fr_ref, wk_hbm, wv_hbm, wq_hbm, q_ref, k_ref, v_ref, slot_ref,
                   lens, wn, hid, xn, wkv, wq, kv, mine, theirs, sem_l, sem_n, sem_h, sem_k, sem_v, sem_q, kv_s, kv_r,
                   x_s, x_r):
    f32, bf16 = jnp.float32, jnp.bfloat16
    rows = hid.shape[0]
    head_dim = wq.shape[2]
    heads, half = wq.shape[0], head_dim // 2
    brows = rows // q_ref.shape[1]
    me = lax.axis_index('sp')
    core = lax.rem(me, 2)
    partner = {'sp': me + 1 - 2 * core}

    def q_copy(j):
        columns = pl.ds(pl.multiple_of((core * heads + j) * head_dim, head_dim), head_dim)
        return pltpu.make_async_copy(wq_hbm.at[:, columns], wq.at[j], sem_q.at[j])

    def exchange(j):
        return pltpu.make_async_remote_copy(src_ref=mine.at[j], dst_ref=theirs.at[j], send_sem=x_s.at[j],
                                            recv_sem=x_r.at[j], device_id=partner, device_id_type=MESH)

    part = pl.ds(pl.multiple_of(core * half, half), half)
    l_copy = pltpu.make_async_copy(len_hbm, lens, sem_l)
    n_copy = pltpu.make_async_copy(wn_hbm, wn, sem_n)
    h_copy = pltpu.make_async_copy(hid_hbm, hid, sem_h)
    k_copy = pltpu.make_async_copy(wk_hbm.at[:, part], wkv.at[:, pl.ds(0, half)], sem_k)
    v_copy = pltpu.make_async_copy(wv_hbm.at[:, part], wkv.at[:, pl.ds(half, half)], sem_v)
    for copy in (h_copy, l_copy, n_copy, k_copy, v_copy):
        copy.start()
    ahead = 5
    for j in range(2):
        q_copy(j).start()
    barrier = pltpu.get_barrier_semaphore()
    pl.semaphore_signal(barrier, inc=1, device_id=partner, device_id_type=MESH)

    l_copy.wait()
    lengths = lens[...].reshape(1, rows)
    across = lax.broadcasted_iota(jnp.int32, (rows, rows), 1)
    down = lax.broadcasted_iota(jnp.int32, (rows, rows), 0)
    column = jnp.sum(jnp.where(across == down, lengths, 0).astype(f32), axis=1, keepdims=True)
    slot = lax.broadcasted_iota(jnp.int32, (rows, slots), 1) + me * slots
    slot_ref[...] = (slot.astype(f32) == column).astype(jnp.int32)
    angles = column * fr_ref[...]
    cos_t, sin_t = jnp.cos(angles), jnp.sin(angles)

    n_copy.wait()
    gain = 1.0 + wn[...].astype(f32).reshape(1, wn.shape[0])
    h_copy.wait()
    for j in range(2, ahead):
        q_copy(j).start()
    x = hid[...].astype(f32)
    inv_rms = lax.rsqrt(jnp.mean(x * x, axis=-1, keepdims=True) + EPSILON)
    xn[...] = (x * inv_rms * gain).astype(bf16)

    def project(w):
        y = jnp.dot(xn[...], w, preferred_element_type=f32)
        return y.astype(bf16)

    k_copy.wait()
    v_copy.wait()
    y = project(wkv[...]).astype(f32)
    kv[core, 0] = y[:, 0:half]
    kv[core, 1] = y[:, half:2 * half]
    pl.semaphore_wait(barrier, 1)
    kv_copy = pltpu.make_async_remote_copy(src_ref=kv.at[core], dst_ref=kv.at[core], send_sem=kv_s, recv_sem=kv_r,
                                           device_id=partner, device_id_type=MESH)
    kv_copy.start()

    def place(k, j, y):
        for i in range(q_ref.shape[1]):
            for d in range(2):
                q_ref[k, i, d, pl.ds(j, brows, stride=heads), :] = y[i * brows:(i + 1) * brows, d * half:(d + 1) * half]

    def one_head(j, carry):
        q_copy(j).wait()

        @pl.when(j + ahead < heads)
        def _():
            q_copy(j + ahead).start()

        y = project(wq[j]).astype(f32)
        mine[j] = (rotate(y, cos_t, sin_t) * head_dim ** -0.5).astype(bf16).astype(f32)
        exchange(j).start()
        place(core, j, mine[j])
        return carry

    lax.fori_loop(0, heads, one_head, 0)
    kv_copy.wait_recv()
    k_ref[...] = rotate(jnp.concatenate([kv[0, 0], kv[1, 0]], axis=-1), cos_t, sin_t).astype(bf16)
    v_ref[...] = jnp.concatenate([kv[0, 1], kv[1, 1]], axis=-1).astype(bf16)

    def their_head(j, carry):
        exchange(j).wait_recv()
        place(1 - core, j, theirs[j])
        return carry

    lax.fori_loop(0, heads, their_head, 0)
    kv_copy.wait_send()

    def finish(j, carry):
        exchange(j).wait_send()
        return carry

    lax.fori_loop(0, heads, finish, 0)


def attend_kernel(len_ref, q_all, kc_ref, vc_ref, hid_ref, wo_hbm, out_ref,
                  p_buf, mine, theirs, r_recv, l_recv, from_left, from_right, att, a_bf, wo, gath, other,
                  sem_wo, d_s, d_r, rs_s, rs_r, at_s, at_r, own_s, own_r, fw_s, fw_r, h_s, h_r):
    f32, bf16 = jnp.float32, jnp.bfloat16
    me = lax.axis_index('sp')
    chip, core = me // 2, lax.rem(me, 2)
    mate = 1 - core
    peers = 2 * CHIPS
    slots = kc_ref.shape[1]
    urows = 2 * CROWS
    hrows = CROWS // 2
    hl = att.shape[4]
    heads = att.shape[3] // CROWS
    hh = heads // 2
    hd = 2 * hl
    nq = wo.shape[0]
    nm = own_s.shape[2]
    per = nq // nm
    data = mine.shape[4] - 8

    def at(c, k):
        return {'sp': lax.rem(c + CHIPS, CHIPS) * 2 + k}

    right, left = at(chip + 1, core), at(chip - 1, core)
    partner = at(chip, mate)

    def remote(src, dst, ssem, rsem, dev):
        return pltpu.make_async_remote_copy(src_ref=src, dst_ref=dst, send_sem=ssem, recv_sem=rsem,
                                            device_id=dev, device_id_type=MESH)

    def wo_copy(j):
        columns = pl.ds(pl.multiple_of((core * nq + j) * hd, hd), hd)
        return pltpu.make_async_copy(wo_hbm.at[:, columns], wo.at[j], sem_wo.at[j])

    for j in range(nq):
        wo_copy(j).start()

    barrier = pltpu.get_barrier_semaphore()
    for dev in (right, left, partner):
        pl.semaphore_signal(barrier, inc=1, device_id=dev, device_id_type=MESH)

    lane = lax.broadcasted_iota(jnp.int32, (heads, slots), 1)
    lane8 = lax.broadcasted_iota(jnp.int32, (8, 128), 1)
    is_max = lane8 < 64
    position = me * slots + lane

    def place_of(t):
        return lax.rem(chip + 2 - t + 3 * (t // 2) - 2 * (t // 3), CHIPS)

    def scores(ph, t):
        i = 2 * place_of(t) + ph
        for kk in range(2):
            for half in range(2):
                stat = jnp.zeros((8, 128), f32)
                for r4 in range(hrows):
                    r = kk * CROWS + half * hrows + r4
                    b = i * urows + r
                    own_rows = slice(r * hh, (r + 1) * hh)
                    q = jnp.concatenate([
                        jnp.concatenate([q_all[k, i, d, own_rows, :] for k in range(2)], axis=0) for d in range(2)], axis=1)
                    s = lax.dot_general(q.astype(bf16), kc_ref[b], (((1,), (1,)), ((), ())), preferred_element_type=f32)
                    valid = position <= len_ref[b]
                    s = jnp.where(valid, s, LOWEST)
                    m = jnp.max(s, axis=1, keepdims=True)
                    p = jnp.where(valid, jnp.exp(s - m), 0.0)
                    den = jnp.sum(p, axis=1, keepdims=True)
                    p_buf[t, r] = p.astype(bf16)
                    for g in range(2):
                        stat = jnp.where(lane8 == g * 32 + r4, m[g * 8:(g + 1) * 8],
                                         jnp.where(lane8 == 64 + g * 32 + r4, den[g * 8:(g + 1) * 8], stat))
                mine[ph, t, kk, half, data:data + 8, :] = stat

    def values(ph, t):
        i = 2 * place_of(t) + ph
        for kk in range(2):
            for half in range(2):
                for r4 in range(hrows):
                    r = kk * CROWS + half * hrows + r4
                    o = jnp.dot(p_buf[t, r], vc_ref[i * urows + r], preferred_element_type=f32)
                    for d in range(2):
                        rows = slice((d * hrows + r4) * heads, (d * hrows + r4 + 1) * heads)
                        mine[ph, t, kk, half, rows, :] = o[:, d * hl:(d + 1) * hl]

    def d_copy(ph, t):
        return remote(mine.at[ph, t, mate], theirs.at[ph, t], d_s.at[ph, t], d_r.at[ph, t], partner)

    def tiles():
        for r4 in range(hrows):
            for g in range(2):
                for d in range(2):
                    yield g * 32 + r4, (d * hrows + r4) * heads + g * 8, d, r4, g

    def merge(into, src):
        one, two = into[data:data + 8, :], src[data:data + 8, :]
        top = jnp.maximum(one, two)
        a, b = jnp.exp(one - top), jnp.exp(two - top)
        den = pltpu.roll(a, 64, 1) * one + pltpu.roll(b, 64, 1) * two
        for column, row, _, _, _ in tiles():
            into[row:row + 8, :] = (into[row:row + 8, :] * a[:, column:column + 1]
                                    + src[row:row + 8, :] * b[:, column:column + 1])
        into[data:data + 8, :] = jnp.where(is_max, top, den)

    def combine(ph, t):
        d_copy(ph, t).wait_recv()
        for half in range(2):
            merge(mine.at[ph, t, core, half], theirs.at[ph, t, half])

    def ring(ph, n, src, dst, dev):
        return remote(src, dst, rs_s.at[ph, n], rs_r.at[ph, n], dev)

    def piece(ph, t, half):
        return mine.at[ph, t, core, half]

    def r1(ph):
        return ring(ph, 0, piece(ph, 0, 0), r_recv.at[ph], right)

    def l1(ph):
        return ring(ph, 1, piece(ph, 0, 1), l_recv.at[ph], left)

    def r2(ph, half):
        return ring(ph, 2 + half, piece(ph, 1, half), from_left.at[ph, half], right)

    def l2(ph, half):
        return ring(ph, 4 + half, piece(ph, 2, half), from_right.at[ph, half], left)

    def reduce_far(ph):
        combine(ph, 0)
        r1(ph).start()
        l1(ph).start()

    def reduce_near(ph):
        combine(ph, 1)
        r2(ph, 1).start()
        combine(ph, 2)
        l2(ph, 0).start()

    def reduce_turn(ph):
        r1(ph).wait_recv()
        merge(piece(ph, 1, 0), r_recv.at[ph])
        r2(ph, 0).start()
        l1(ph).wait_recv()
        merge(piece(ph, 2, 1), l_recv.at[ph])
        l2(ph, 1).start()

    def at_copy(ph):
        return remote(att.at[ph, core], att.at[ph, core], at_s.at[ph], at_r.at[ph], partner)

    def reduce_end(ph):
        for half in range(2):
            r2(ph, half).wait_recv()
            l2(ph, half).wait_recv()
            parts = [mine.at[ph, 3, core, half], from_left.at[ph, half], from_right.at[ph, half]]
            stats = [x[data:data + 8, :] for x in parts]
            top = jnp.maximum(jnp.maximum(stats[0], stats[1]), stats[2])
            scale = [jnp.exp(x - top) for x in stats]
            den = sum(a * pltpu.roll(x, 64, 1) for a, x in zip(scale, stats))
            den = jnp.where(is_max & (lane8 % 32 < hrows), den, 1.0)
            scale = [a / den for a in scale]
            for column, row, d, r4, g in tiles():
                y = sum(x[row:row + 8, :] * a[:, column:column + 1] for x, a in zip(parts, scale))
                to = (half * hrows + r4) * heads + g * 8
                att[ph, core, d, to:to + 8, :] = y
        at_copy(ph).start()

    def rows_of(c, ph):
        return pl.ds(pl.multiple_of((2 * c + ph) * urows, urows), urows)

    def columns_of(k, n):
        return pl.ds(pl.multiple_of((k * nq + n) * hd, hd), hd)

    def own_copies(ph, u):
        src = gath.at[ph, chip, pl.ds(u * per, per)]
        return (remote(src, src, own_s.at[ph, 0, u], own_r.at[ph, 0, u], right),
                remote(src, src, own_s.at[ph, 1, u], own_r.at[ph, 1, u], left),
                to_mate(ph, 0, chip, u))

    def to_mate(ph, which, c, u):
        part = pl.ds(u * per, per)
        return remote(gath.at[ph, c, part], other.at[ph, c, part], h_s.at[ph, which, u], h_r.at[ph, which, u], partner)

    def gather_rows(ph):
        at_copy(ph).wait_recv()
        for h in range(heads):
            for d in range(2):
                pair = [att[ph, kk, d, pl.ds(h, CROWS, stride=heads), :] for kk in range(2)]
                a_bf[ph, :, h * hd + d * hl:h * hd + (d + 1) * hl] = jnp.concatenate(pair, axis=0).astype(bf16)

    def project(ph, u):
        for n in range(u * per, (u + 1) * per):
            if ph == 0:
                wo_copy(n).wait()
            y = jnp.dot(a_bf[ph], wo[n], preferred_element_type=f32)
            gath[ph, chip, n] = hid_ref[rows_of(chip, ph), columns_of(core, n)].astype(f32) + y
        for copy in own_copies(ph, u):
            copy.start()

    cl, cr, co = place_of(2), place_of(1), place_of(0)
    split = nm // 2

    def forward(ph, u):
        c, dev = (cl, right) if u < split else (cr, left)
        src = gath.at[ph, c, pl.ds(u * per, per)]
        return remote(src, src, fw_s.at[ph, u], fw_r.at[ph, u], dev)

    def put(ph, c, u):
        for n in range(u * per, (u + 1) * per):
            out_ref[rows_of(c, ph), columns_of(core, n)] = gath[ph, c, n].astype(bf16)

    def put_other(ph, c, u):
        for n in range(u * per, (u + 1) * per):
            out_ref[rows_of(c, ph), columns_of(mate, n)] = other[ph, c, n].astype(bf16)

    def relay(ph, u):
        own_copies(ph, u)[0].wait_recv()
        if u < split:
            forward(ph, u).start()
        to_mate(ph, 1, cl, u).start()
        own_copies(ph, u)[1].wait_recv()
        if u >= split:
            forward(ph, u).start()
        to_mate(ph, 2, cr, u).start()

    def relay_end(ph):
        for u in range(nm):
            forward(ph, u).wait_recv()
            to_mate(ph, 3, co, u).start()

    places = ((0, chip), (1, cl), (2, cr), (3, co))

    def finish(ph):
        for which, c in places:
            for u in range(nm):
                put(ph, c, u)
                to_mate(ph, which, c, u).wait_recv()
                put_other(ph, c, u)

    def scores_of(ph):
        def body(t, carry):
            scores(ph, t)
            return carry

        lax.fori_loop(0, CHIPS, body, 0)

    def values_of(ph):
        def body(t, carry):
            values(ph, t)
            d_copy(ph, t).start()
            return carry

        lax.fori_loop(0, CHIPS, body, 0)

    scores_of(0)
    pl.semaphore_wait(barrier, 3)
    values_of(0)
    scores_of(1)
    reduce_far(0)
    reduce_near(0)
    values_of(1)
    reduce_far(1)
    reduce_turn(0)
    reduce_near(1)
    combine(0, 3)
    combine(1, 3)
    reduce_turn(1)
    reduce_end(0)
    gather_rows(0)
    for u in range(split):
        project(0, u)
    reduce_end(1)
    for u in range(split, nm):
        project(0, u)
    gather_rows(1)
    for u in range(nm):
        project(1, u)
        relay(0, u)
    for u in range(split):
        relay(1, u)
    relay_end(0)
    for u in range(split, nm):
        relay(1, u)
    finish(0)
    relay_end(1)
    finish(1)

    for ph in range(2):
        for t in range(CHIPS):
            d_copy(ph, t).wait_send()
        for copy in (r1(ph), l1(ph), r2(ph, 0), r2(ph, 1), l2(ph, 0), l2(ph, 1), at_copy(ph)):
            copy.wait_send()
        for u in range(nm):
            for copy in own_copies(ph, u):
                copy.wait_send()
            forward(ph, u).wait_send()
            for which, c in places[1:]:
                to_mate(ph, which, c, u).wait_send()


def local_step(hidden, w_norm, w_q, w_k, w_v, w_o, k_block, v_block, cache_len):
    f32, bf16 = jnp.float32, jnp.bfloat16
    rows, width = hidden.shape
    seq_block, hd = k_block.shape[1], k_block.shape[2]
    heads = w_q.shape[1] // hd
    hh, hl = heads // 2, hd // 2
    nblk = 2 * CHIPS
    brows = rows // nblk
    assert brows == 2 * CROWS
    inv_freq = (ROPE_BASE ** (-jnp.arange(hl, dtype=f32) * 2.0 / hd)).reshape(1, hl)
    vmem = pl.BlockSpec(memory_space=pltpu.VMEM)
    hbm = pl.BlockSpec(memory_space=pl.ANY)
    smem = pl.BlockSpec(memory_space=pltpu.SMEM)
    dma = pltpu.SemaphoreType.DMA

    def keep(x):
        return pltpu.with_memory_space_constraint(x, pltpu.HBM)

    def near(x):
        return pltpu.with_memory_space_constraint(x, pltpu.VMEM)

    q_all, k_rot, v_new, slot = pl.pallas_call(
        functools.partial(project_kernel, seq_block),
        out_shape=(pltpu.VMEM((2, nblk, 2, brows * hh, hl), f32), jax.ShapeDtypeStruct((rows, hd), bf16),
                   jax.ShapeDtypeStruct((rows, hd), bf16), jax.ShapeDtypeStruct((rows, seq_block), jnp.int32)),
        in_specs=[hbm] * 3 + [vmem] + [hbm] * 3,
        out_specs=(vmem,) * 4,
        scratch_shapes=[
            pltpu.VMEM((rows,), jnp.int32),
            pltpu.VMEM((width,), bf16),
            pltpu.VMEM((rows, width), bf16),
            pltpu.VMEM((rows, width), bf16),
            pltpu.VMEM((width, hd), bf16),
            pltpu.VMEM((hh, width, hd), bf16),
            pltpu.VMEM((2, 2, rows, hl), f32),
            pltpu.VMEM((hh, rows, hd), f32),
            pltpu.VMEM((hh, rows, hd), f32),
            dma, dma, dma, dma, dma, dma((hh,)), dma, dma, dma((hh,)), dma((hh,)),
        ],
        compiler_params=pltpu.CompilerParams(collective_id=1, has_side_effects=True, vmem_limit_bytes=48 * MIB),
        cost_estimate=pl.CostEstimate(flops=2 * rows * width * (hh + 1) * hd, bytes_accessed=2 * width * (hh + 1) * hd,
                                      transcendentals=0),
        name='project',
    )(keep(cache_len), keep(hidden), keep(w_norm), inv_freq, keep(w_k), keep(w_v), keep(w_q))

    at_slot = (slot != 0)[:, :, None]
    new_k_block = jnp.where(at_slot, k_rot[:, None, :], k_block)
    new_v_block = jnp.where(at_slot, v_new[:, None, :], v_block)

    half_rows = CROWS * heads + 8
    nm = hh // 2
    out_hidden = pl.pallas_call(
        attend_kernel,
        out_shape=jax.ShapeDtypeStruct((rows, width), bf16),
        in_specs=[smem, vmem, vmem, vmem, vmem, hbm],
        out_specs=vmem,
        scratch_shapes=[
            pltpu.VMEM((CHIPS, brows, heads, seq_block), bf16),
            pltpu.VMEM((2, CHIPS, 2, 2, half_rows, hl), f32),
            pltpu.VMEM((2, CHIPS, 2, half_rows, hl), f32),
            pltpu.VMEM((2, half_rows, hl), f32),
            pltpu.VMEM((2, half_rows, hl), f32),
            pltpu.VMEM((2, 2, half_rows, hl), f32),
            pltpu.VMEM((2, 2, half_rows, hl), f32),
            pltpu.VMEM((2, 2, 2, CROWS * heads, hl), f32),
            pltpu.VMEM((2, brows, width), bf16),
            pltpu.VMEM((hh, width, hd), bf16),
            pltpu.VMEM((2, CHIPS, hh, brows, hd), f32),
            pltpu.VMEM((2, CHIPS, hh, brows, hd), f32),
            dma((hh,)), dma((2, CHIPS)), dma((2, CHIPS)), dma((2, 6)), dma((2, 6)), dma((2,)), dma((2,)),
            dma((2, 2, nm)), dma((2, 2, nm)), dma((2, nm)), dma((2, nm)), dma((2, CHIPS, nm)), dma((2, CHIPS, nm)),
        ],
        compiler_params=pltpu.CompilerParams(collective_id=0, has_side_effects=True, vmem_limit_bytes=26 * MIB),
        cost_estimate=pl.CostEstimate(flops=2 * rows * width * hh * hd * 2, bytes_accessed=2 * width * hh * hd,
                                      transcendentals=0),
        name='attend',
    )(cache_len, near(q_all), near(new_k_block), near(new_v_block), hidden, keep(w_o))
    return out_hidden, new_k_block, new_v_block


def solution(mesh):
    assert mesh.shape['sp'] == 2 * CHIPS
    cache_spec = P('dp', 'sp', None)
    return jax.shard_map(local_step, mesh=mesh, in_specs=(P('dp', None), P(None), P(None, None), P(None, None), P(None, None), P(None, None), cache_spec, cache_spec, P('dp')), out_specs=(P('dp', None), cache_spec, cache_spec), check_vma=False)
```

```python
import functools

import jax
import jax.numpy as jnp
from jax import lax
from jax.experimental import pallas as pl
from jax.experimental.pallas import tpu as pltpu
from jax.sharding import PartitionSpec as P

ROPE_BASE = 10000.0
EPSILON = 1e-6
MESH = pl.DeviceIdType.MESH
MIB = 1 << 20
LOWEST = float(jnp.finfo(jnp.float32).min)
CROWS = 8
CHIPS = 4


def rotate(x, cos_t, sin_t):
    half = x.shape[-1] // 2
    low, high = x[:, :half], x[:, half:]
    return jnp.concatenate([low * cos_t - high * sin_t, high * cos_t + low * sin_t], axis=-1)


def project_kernel(slots, len_hbm, hid_hbm, wn_hbm, fr_ref, wk_hbm, wv_hbm, wq_hbm, q_ref, k_ref, v_ref, slot_ref,
                   lens, wn, hid, xn, wkv, wq, kv, mine, theirs, sem_l, sem_n, sem_h, sem_k, sem_v, sem_q, kv_s, kv_r,
                   x_s, x_r):
    f32, bf16 = jnp.float32, jnp.bfloat16
    rows = hid.shape[0]
    head_dim = wq.shape[2]
    heads, half = wq.shape[0], head_dim // 2
    brows = rows // q_ref.shape[1]
    me = lax.axis_index('sp')
    core = lax.rem(me, 2)
    partner = {'sp': me + 1 - 2 * core}

    def q_copy(j):
        columns = pl.ds(pl.multiple_of((core * heads + j) * head_dim, head_dim), head_dim)
        return pltpu.make_async_copy(wq_hbm.at[:, columns], wq.at[j], sem_q.at[j])

    def exchange(j):
        return pltpu.make_async_remote_copy(src_ref=mine.at[j], dst_ref=theirs.at[j], send_sem=x_s.at[j],
                                            recv_sem=x_r.at[j], device_id=partner, device_id_type=MESH)

    part = pl.ds(pl.multiple_of(core * half, half), half)
    l_copy = pltpu.make_async_copy(len_hbm, lens, sem_l)
    n_copy = pltpu.make_async_copy(wn_hbm, wn, sem_n)
    h_copy = pltpu.make_async_copy(hid_hbm, hid, sem_h)
    k_copy = pltpu.make_async_copy(wk_hbm.at[:, part], wkv.at[:, pl.ds(0, half)], sem_k)
    v_copy = pltpu.make_async_copy(wv_hbm.at[:, part], wkv.at[:, pl.ds(half, half)], sem_v)
    for copy in (h_copy, l_copy, n_copy, k_copy, v_copy):
        copy.start()
    ahead = 5
    for j in range(2):
        q_copy(j).start()
    barrier = pltpu.get_barrier_semaphore()
    pl.semaphore_signal(barrier, inc=1, device_id=partner, device_id_type=MESH)

    l_copy.wait()
    lengths = lens[...].reshape(1, rows)
    across = lax.broadcasted_iota(jnp.int32, (rows, rows), 1)
    down = lax.broadcasted_iota(jnp.int32, (rows, rows), 0)
    column = jnp.sum(jnp.where(across == down, lengths, 0).astype(f32), axis=1, keepdims=True)
    slot = lax.broadcasted_iota(jnp.int32, (rows, slots), 1) + me * slots
    slot_ref[...] = (slot.astype(f32) == column).astype(jnp.int32)
    angles = column * fr_ref[...]
    cos_t, sin_t = jnp.cos(angles), jnp.sin(angles)

    n_copy.wait()
    gain = 1.0 + wn[...].astype(f32).reshape(1, wn.shape[0])
    h_copy.wait()
    for j in range(2, ahead):
        q_copy(j).start()
    x = hid[...].astype(f32)
    inv_rms = lax.rsqrt(jnp.mean(x * x, axis=-1, keepdims=True) + EPSILON)
    xn[...] = (x * inv_rms * gain).astype(bf16)

    def project(w):
        y = jnp.dot(xn[...], w, preferred_element_type=f32)
        return y.astype(bf16)

    k_copy.wait()
    v_copy.wait()
    y = project(wkv[...]).astype(f32)
    kv[core, 0] = y[:, 0:half]
    kv[core, 1] = y[:, half:2 * half]
    pl.semaphore_wait(barrier, 1)
    kv_copy = pltpu.make_async_remote_copy(src_ref=kv.at[core], dst_ref=kv.at[core], send_sem=kv_s, recv_sem=kv_r,
                                           device_id=partner, device_id_type=MESH)
    kv_copy.start()

    def place(k, j, y):
        for i in range(q_ref.shape[1]):
            for d in range(2):
                q_ref[k, i, d, pl.ds(j, brows, stride=heads), :] = y[i * brows:(i + 1) * brows, d * half:(d + 1) * half]

    def one_head(j, carry):
        q_copy(j).wait()

        @pl.when(j + ahead < heads)
        def _():
            q_copy(j + ahead).start()

        y = project(wq[j]).astype(f32)
        mine[j] = (rotate(y, cos_t, sin_t) * head_dim ** -0.5).astype(bf16).astype(f32)
        exchange(j).start()
        place(core, j, mine[j])
        return carry

    lax.fori_loop(0, heads, one_head, 0)
    kv_copy.wait_recv()
    k_ref[...] = rotate(jnp.concatenate([kv[0, 0], kv[1, 0]], axis=-1), cos_t, sin_t).astype(bf16)
    v_ref[...] = jnp.concatenate([kv[0, 1], kv[1, 1]], axis=-1).astype(bf16)

    def their_head(j, carry):
        exchange(j).wait_recv()
        place(1 - core, j, theirs[j])
        return carry

    lax.fori_loop(0, heads, their_head, 0)
    kv_copy.wait_send()

    def finish(j, carry):
        exchange(j).wait_send()
        return carry

    lax.fori_loop(0, heads, finish, 0)


def attend_kernel(len_ref, q_all, kc_ref, vc_ref, hid_ref, wo_hbm, out_ref,
                  p_buf, mine, theirs, r_recv, l_recv, from_left, from_right, att, a_bf, wo, gath, other,
                  sem_wo, d_s, d_r, rs_s, rs_r, at_s, at_r, own_s, own_r, fw_s, fw_r, h_s, h_r):
    f32, bf16 = jnp.float32, jnp.bfloat16
    me = lax.axis_index('sp')
    chip, core = me // 2, lax.rem(me, 2)
    mate = 1 - core
    peers = 2 * CHIPS
    slots = kc_ref.shape[1]
    urows = 2 * CROWS
    hrows = CROWS // 2
    hl = att.shape[4]
    heads = att.shape[3] // CROWS
    hh = heads // 2
    hd = 2 * hl
    nq = wo.shape[0]
    nm = own_s.shape[2]
    per = nq // nm
    data = mine.shape[4] - 8

    def at(c, k):
        return {'sp': lax.rem(c + CHIPS, CHIPS) * 2 + k}

    right, left = at(chip + 1, core), at(chip - 1, core)
    partner = at(chip, mate)

    def remote(src, dst, ssem, rsem, dev):
        return pltpu.make_async_remote_copy(src_ref=src, dst_ref=dst, send_sem=ssem, recv_sem=rsem,
                                            device_id=dev, device_id_type=MESH)

    def wo_copy(j):
        columns = pl.ds(pl.multiple_of((core * nq + j) * hd, hd), hd)
        return pltpu.make_async_copy(wo_hbm.at[:, columns], wo.at[j], sem_wo.at[j])

    for j in range(nq):
        wo_copy(j).start()

    barrier = pltpu.get_barrier_semaphore()
    for dev in (right, left, partner):
        pl.semaphore_signal(barrier, inc=1, device_id=dev, device_id_type=MESH)

    lane = lax.broadcasted_iota(jnp.int32, (heads, slots), 1)
    lane8 = lax.broadcasted_iota(jnp.int32, (8, 128), 1)
    is_max = lane8 < 64
    position = me * slots + lane

    def place_of(t):
        return lax.rem(chip + 2 - t + 3 * (t // 2) - 2 * (t // 3), CHIPS)

    def scores(ph, t):
        i = 2 * place_of(t) + ph
        for kk in range(2):
            for half in range(2):
                stat = jnp.zeros((8, 128), f32)
                for r4 in range(hrows):
                    r = kk * CROWS + half * hrows + r4
                    b = i * urows + r
                    own_rows = slice(r * hh, (r + 1) * hh)
                    q = jnp.concatenate([
                        jnp.concatenate([q_all[k, i, d, own_rows, :] for k in range(2)], axis=0) for d in range(2)], axis=1)
                    s = lax.dot_general(q.astype(bf16), kc_ref[b], (((1,), (1,)), ((), ())), preferred_element_type=f32)
                    valid = position <= len_ref[b]
                    s = jnp.where(valid, s, LOWEST)
                    m = jnp.max(s, axis=1, keepdims=True)
                    p = jnp.where(valid, jnp.exp(s - m), 0.0)
                    den = jnp.sum(p, axis=1, keepdims=True)
                    p_buf[t, r] = p.astype(bf16)
                    for g in range(2):
                        stat = jnp.where(lane8 == g * 32 + r4, m[g * 8:(g + 1) * 8],
                                         jnp.where(lane8 == 64 + g * 32 + r4, den[g * 8:(g + 1) * 8], stat))
                mine[ph, t, kk, half, data:data + 8, :] = stat

    def values(ph, t):
        i = 2 * place_of(t) + ph
        for kk in range(2):
            for half in range(2):
                for r4 in range(hrows):
                    r = kk * CROWS + half * hrows + r4
                    o = jnp.dot(p_buf[t, r], vc_ref[i * urows + r], preferred_element_type=f32)
                    for d in range(2):
                        rows = slice((d * hrows + r4) * heads, (d * hrows + r4 + 1) * heads)
                        mine[ph, t, kk, half, rows, :] = o[:, d * hl:(d + 1) * hl]

    def d_copy(ph, t):
        return remote(mine.at[ph, t, mate], theirs.at[ph, t], d_s.at[ph, t], d_r.at[ph, t], partner)

    def tiles():
        for r4 in range(hrows):
            for g in range(2):
                for d in range(2):
                    yield g * 32 + r4, (d * hrows + r4) * heads + g * 8, d, r4, g

    def merge(into, src):
        one, two = into[data:data + 8, :], src[data:data + 8, :]
        top = jnp.maximum(one, two)
        a, b = jnp.exp(one - top), jnp.exp(two - top)
        den = pltpu.roll(a, 64, 1) * one + pltpu.roll(b, 64, 1) * two
        for column, row, _, _, _ in tiles():
            into[row:row + 8, :] = (into[row:row + 8, :] * a[:, column:column + 1]
                                    + src[row:row + 8, :] * b[:, column:column + 1])
        into[data:data + 8, :] = jnp.where(is_max, top, den)

    def combine(ph, t):
        d_copy(ph, t).wait_recv()
        for half in range(2):
            merge(mine.at[ph, t, core, half], theirs.at[ph, t, half])

    def ring(ph, n, src, dst, dev):
        return remote(src, dst, rs_s.at[ph, n], rs_r.at[ph, n], dev)

    def piece(ph, t, half):
        return mine.at[ph, t, core, half]

    def r1(ph):
        return ring(ph, 0, piece(ph, 0, 0), r_recv.at[ph], right)

    def l1(ph):
        return ring(ph, 1, piece(ph, 0, 1), l_recv.at[ph], left)

    def r2(ph, half):
        return ring(ph, 2 + half, piece(ph, 1, half), from_left.at[ph, half], right)

    def l2(ph, half):
        return ring(ph, 4 + half, piece(ph, 2, half), from_right.at[ph, half], left)

    def reduce_far(ph):
        combine(ph, 0)
        r1(ph).start()
        l1(ph).start()

    def reduce_near(ph):
        combine(ph, 1)
        r2(ph, 1).start()
        combine(ph, 2)
        l2(ph, 0).start()

    def reduce_turn(ph):
        r1(ph).wait_recv()
        merge(piece(ph, 1, 0), r_recv.at[ph])
        r2(ph, 0).start()
        l1(ph).wait_recv()
        merge(piece(ph, 2, 1), l_recv.at[ph])
        l2(ph, 1).start()

    def at_copy(ph):
        return remote(att.at[ph, core], att.at[ph, core], at_s.at[ph], at_r.at[ph], partner)

    def reduce_end(ph):
        for half in range(2):
            r2(ph, half).wait_recv()
            l2(ph, half).wait_recv()
            parts = [mine.at[ph, 3, core, half], from_left.at[ph, half], from_right.at[ph, half]]
            stats = [x[data:data + 8, :] for x in parts]
            top = jnp.maximum(jnp.maximum(stats[0], stats[1]), stats[2])
            scale = [jnp.exp(x - top) for x in stats]
            den = sum(a * pltpu.roll(x, 64, 1) for a, x in zip(scale, stats))
            den = jnp.where(is_max & (lane8 % 32 < hrows), den, 1.0)
            scale = [a / den for a in scale]
            for column, row, d, r4, g in tiles():
                y = sum(x[row:row + 8, :] * a[:, column:column + 1] for x, a in zip(parts, scale))
                to = (half * hrows + r4) * heads + g * 8
                att[ph, core, d, to:to + 8, :] = y
        at_copy(ph).start()

    def rows_of(c, ph):
        return pl.ds(pl.multiple_of((2 * c + ph) * urows, urows), urows)

    def columns_of(k, n):
        return pl.ds(pl.multiple_of((k * nq + n) * hd, hd), hd)

    def own_copies(ph, u):
        src = gath.at[ph, chip, pl.ds(u * per, per)]
        return (remote(src, src, own_s.at[ph, 0, u], own_r.at[ph, 0, u], right),
                remote(src, src, own_s.at[ph, 1, u], own_r.at[ph, 1, u], left),
                to_mate(ph, 0, chip, u))

    def to_mate(ph, which, c, u):
        part = pl.ds(u * per, per)
        return remote(gath.at[ph, c, part], other.at[ph, c, part], h_s.at[ph, which, u], h_r.at[ph, which, u], partner)

    def gather_rows(ph):
        at_copy(ph).wait_recv()
        for h in range(heads):
            for d in range(2):
                pair = [att[ph, kk, d, pl.ds(h, CROWS, stride=heads), :] for kk in range(2)]
                a_bf[ph, :, h * hd + d * hl:h * hd + (d + 1) * hl] = jnp.concatenate(pair, axis=0).astype(bf16)

    def project(ph, u):
        for n in range(u * per, (u + 1) * per):
            if ph == 0:
                wo_copy(n).wait()
            y = jnp.dot(a_bf[ph], wo[n], preferred_element_type=f32)
            gath[ph, chip, n] = hid_ref[rows_of(chip, ph), columns_of(core, n)].astype(f32) + y
        for copy in own_copies(ph, u):
            copy.start()

    cl, cr, co = place_of(2), place_of(1), place_of(0)
    split = nm // 2

    def forward(ph, u):
        c, dev = (cl, right) if u < split else (cr, left)
        src = gath.at[ph, c, pl.ds(u * per, per)]
        return remote(src, src, fw_s.at[ph, u], fw_r.at[ph, u], dev)

    def put(ph, c, u):
        for n in range(u * per, (u + 1) * per):
            out_ref[rows_of(c, ph), columns_of(core, n)] = gath[ph, c, n].astype(bf16)

    def put_other(ph, c, u):
        for n in range(u * per, (u + 1) * per):
            out_ref[rows_of(c, ph), columns_of(mate, n)] = other[ph, c, n].astype(bf16)

    def relay(ph, u):
        own_copies(ph, u)[0].wait_recv()
        if u < split:
            forward(ph, u).start()
        to_mate(ph, 1, cl, u).start()
        own_copies(ph, u)[1].wait_recv()
        if u >= split:
            forward(ph, u).start()
        to_mate(ph, 2, cr, u).start()

    def relay_end(ph):
        for u in range(nm):
            forward(ph, u).wait_recv()
            to_mate(ph, 3, co, u).start()

    places = ((0, chip), (1, cl), (2, cr), (3, co))

    def finish(ph):
        for which, c in places:
            for u in range(nm):
                put(ph, c, u)
                to_mate(ph, which, c, u).wait_recv()
                put_other(ph, c, u)

    def units(ph, first, last, send):
        def body(t, carry):
            scores(ph, t)
            values(ph, t)
            if send:
                d_copy(ph, t).start()
            return carry

        lax.fori_loop(first, last, body, 0)

    units(0, 0, 2, False)
    pl.semaphore_wait(barrier, 3)
    d_copy(0, 0).start()
    d_copy(0, 1).start()
    units(0, 2, CHIPS, True)
    reduce_far(0)
    reduce_near(0)
    units(1, 0, CHIPS, True)
    reduce_far(1)
    reduce_turn(0)
    reduce_near(1)
    combine(0, 3)
    reduce_turn(1)
    combine(1, 3)
    reduce_end(0)
    gather_rows(0)
    for u in range(split):
        project(0, u)
    reduce_end(1)
    for u in range(split, nm):
        project(0, u)
    for u in range(split):
        relay(0, u)
    gather_rows(1)
    for u in range(nm):
        project(1, u)
        if u < nm - split:
            relay(0, split + u)
    for u in range(split):
        relay(1, u)
    relay_end(0)
    for u in range(split, nm):
        relay(1, u)
    finish(0)
    relay_end(1)
    finish(1)

    for ph in range(2):
        for t in range(CHIPS):
            d_copy(ph, t).wait_send()
        for copy in (r1(ph), l1(ph), r2(ph, 0), r2(ph, 1), l2(ph, 0), l2(ph, 1), at_copy(ph)):
            copy.wait_send()
        for u in range(nm):
            for copy in own_copies(ph, u):
                copy.wait_send()
            forward(ph, u).wait_send()
            for which, c in places[1:]:
                to_mate(ph, which, c, u).wait_send()


def local_step(hidden, w_norm, w_q, w_k, w_v, w_o, k_block, v_block, cache_len):
    f32, bf16 = jnp.float32, jnp.bfloat16
    rows, width = hidden.shape
    seq_block, hd = k_block.shape[1], k_block.shape[2]
    heads = w_q.shape[1] // hd
    hh, hl = heads // 2, hd // 2
    nblk = 2 * CHIPS
    brows = rows // nblk
    assert brows == 2 * CROWS
    inv_freq = (ROPE_BASE ** (-jnp.arange(hl, dtype=f32) * 2.0 / hd)).reshape(1, hl)
    vmem = pl.BlockSpec(memory_space=pltpu.VMEM)
    hbm = pl.BlockSpec(memory_space=pl.ANY)
    smem = pl.BlockSpec(memory_space=pltpu.SMEM)
    dma = pltpu.SemaphoreType.DMA

    def keep(x):
        return pltpu.with_memory_space_constraint(x, pltpu.HBM)

    def near(x):
        return pltpu.with_memory_space_constraint(x, pltpu.VMEM)

    q_all, k_rot, v_new, slot = pl.pallas_call(
        functools.partial(project_kernel, seq_block),
        out_shape=(pltpu.VMEM((2, nblk, 2, brows * hh, hl), f32), jax.ShapeDtypeStruct((rows, hd), bf16),
                   jax.ShapeDtypeStruct((rows, hd), bf16), jax.ShapeDtypeStruct((rows, seq_block), jnp.int32)),
        in_specs=[hbm] * 3 + [vmem] + [hbm] * 3,
        out_specs=(vmem,) * 4,
        scratch_shapes=[
            pltpu.VMEM((rows,), jnp.int32),
            pltpu.VMEM((width,), bf16),
            pltpu.VMEM((rows, width), bf16),
            pltpu.VMEM((rows, width), bf16),
            pltpu.VMEM((width, hd), bf16),
            pltpu.VMEM((hh, width, hd), bf16),
            pltpu.VMEM((2, 2, rows, hl), f32),
            pltpu.VMEM((hh, rows, hd), f32),
            pltpu.VMEM((hh, rows, hd), f32),
            dma, dma, dma, dma, dma, dma((hh,)), dma, dma, dma((hh,)), dma((hh,)),
        ],
        compiler_params=pltpu.CompilerParams(collective_id=1, has_side_effects=True, vmem_limit_bytes=48 * MIB),
        cost_estimate=pl.CostEstimate(flops=2 * rows * width * (hh + 1) * hd, bytes_accessed=2 * width * (hh + 1) * hd,
                                      transcendentals=0),
        name='project',
    )(keep(cache_len), keep(hidden), keep(w_norm), inv_freq, keep(w_k), keep(w_v), keep(w_q))

    at_slot = (slot != 0)[:, :, None]
    new_k_block = jnp.where(at_slot, k_rot[:, None, :], k_block)
    new_v_block = jnp.where(at_slot, v_new[:, None, :], v_block)

    half_rows = CROWS * heads + 8
    nm = hh // 2
    out_hidden = pl.pallas_call(
        attend_kernel,
        out_shape=jax.ShapeDtypeStruct((rows, width), bf16),
        in_specs=[smem, vmem, vmem, vmem, vmem, hbm],
        out_specs=vmem,
        scratch_shapes=[
            pltpu.VMEM((CHIPS, brows, heads, seq_block), bf16),
            pltpu.VMEM((2, CHIPS, 2, 2, half_rows, hl), f32),
            pltpu.VMEM((2, CHIPS, 2, half_rows, hl), f32),
            pltpu.VMEM((2, half_rows, hl), f32),
            pltpu.VMEM((2, half_rows, hl), f32),
            pltpu.VMEM((2, 2, half_rows, hl), f32),
            pltpu.VMEM((2, 2, half_rows, hl), f32),
            pltpu.VMEM((2, 2, 2, CROWS * heads, hl), f32),
            pltpu.VMEM((2, brows, width), bf16),
            pltpu.VMEM((hh, width, hd), bf16),
            pltpu.VMEM((2, CHIPS, hh, brows, hd), f32),
            pltpu.VMEM((2, CHIPS, hh, brows, hd), f32),
            dma((hh,)), dma((2, CHIPS)), dma((2, CHIPS)), dma((2, 6)), dma((2, 6)), dma((2,)), dma((2,)),
            dma((2, 2, nm)), dma((2, 2, nm)), dma((2, nm)), dma((2, nm)), dma((2, CHIPS, nm)), dma((2, CHIPS, nm)),
        ],
        compiler_params=pltpu.CompilerParams(collective_id=0, has_side_effects=True, vmem_limit_bytes=26 * MIB),
        cost_estimate=pl.CostEstimate(flops=2 * rows * width * hh * hd * 2, bytes_accessed=2 * width * hh * hd,
                                      transcendentals=0),
        name='attend',
    )(cache_len, near(q_all), near(new_k_block), near(new_v_block), hidden, keep(w_o))
    return out_hidden, new_k_block, new_v_block


def solution(mesh):
    assert mesh.shape['sp'] == 2 * CHIPS
    cache_spec = P('dp', 'sp', None)
    return jax.shard_map(local_step, mesh=mesh, in_specs=(P('dp', None), P(None), P(None, None), P(None, None), P(None, None), P(None, None), cache_spec, cache_spec, P('dp')), out_specs=(P('dp', None), cache_spec, cache_spec), check_vma=False)
```

```python
import functools

import jax
import jax.numpy as jnp
from jax import lax
from jax.experimental import pallas as pl
from jax.experimental.pallas import tpu as pltpu
from jax.sharding import PartitionSpec as P

ROPE_BASE = 10000.0
EPSILON = 1e-6
MESH = pl.DeviceIdType.MESH
MIB = 1 << 20
LOWEST = float(jnp.finfo(jnp.float32).min)
CROWS = 8
CHIPS = 4


def rotate(x, cos_t, sin_t):
    half = x.shape[-1] // 2
    low, high = x[:, :half], x[:, half:]
    return jnp.concatenate([low * cos_t - high * sin_t, high * cos_t + low * sin_t], axis=-1)


def project_kernel(slots, len_hbm, hid_hbm, wn_hbm, fr_ref, wk_hbm, wv_hbm, wq_hbm, q_ref, k_ref, v_ref, slot_ref, last_ref,
                   lens, wn, hid, xn, wkv, wq, kv, mine, theirs, sem_l, sem_n, sem_h, sem_k, sem_v, sem_q, kv_s, kv_r,
                   x_s, x_r):
    f32, bf16 = jnp.float32, jnp.bfloat16
    rows = hid.shape[0]
    head_dim = wq.shape[2]
    heads, half = wq.shape[0], head_dim // 2
    brows = rows // q_ref.shape[1]
    me = lax.axis_index('sp')
    core = lax.rem(me, 2)
    partner = {'sp': me + 1 - 2 * core}

    def q_copy(j):
        columns = pl.ds(pl.multiple_of((core * heads + j) * head_dim, head_dim), head_dim)
        return pltpu.make_async_copy(wq_hbm.at[:, columns], wq.at[j], sem_q.at[j])

    def exchange(j):
        return pltpu.make_async_remote_copy(src_ref=mine.at[j], dst_ref=theirs.at[j], send_sem=x_s.at[j],
                                            recv_sem=x_r.at[j], device_id=partner, device_id_type=MESH)

    part = pl.ds(pl.multiple_of(core * half, half), half)
    l_copy = pltpu.make_async_copy(len_hbm, lens, sem_l)
    n_copy = pltpu.make_async_copy(wn_hbm, wn, sem_n)
    h_copy = pltpu.make_async_copy(hid_hbm, hid, sem_h)
    k_copy = pltpu.make_async_copy(wk_hbm.at[:, part], wkv.at[:, pl.ds(0, half)], sem_k)
    v_copy = pltpu.make_async_copy(wv_hbm.at[:, part], wkv.at[:, pl.ds(half, half)], sem_v)
    for copy in (h_copy, l_copy, n_copy, k_copy, v_copy):
        copy.start()
    ahead = 5
    for j in range(2):
        q_copy(j).start()
    barrier = pltpu.get_barrier_semaphore()
    pl.semaphore_signal(barrier, inc=1, device_id=partner, device_id_type=MESH)

    l_copy.wait()
    lengths = lens[...].reshape(1, rows)
    across = lax.broadcasted_iota(jnp.int32, (rows, rows), 1)
    down = lax.broadcasted_iota(jnp.int32, (rows, rows), 0)
    column = jnp.sum(jnp.where(across == down, lengths, 0).astype(f32), axis=1, keepdims=True)
    slot = lax.broadcasted_iota(jnp.int32, (rows, slots), 1) + me * slots
    slot_ref[...] = (slot.astype(f32) == column).astype(jnp.int32)
    last_ref[...] = jnp.broadcast_to(column.astype(jnp.int32) - me * slots, last_ref.shape)
    angles = column * fr_ref[...]
    cos_t, sin_t = jnp.cos(angles), jnp.sin(angles)

    n_copy.wait()
    gain = 1.0 + wn[...].astype(f32).reshape(1, wn.shape[0])
    h_copy.wait()
    for j in range(2, ahead):
        q_copy(j).start()
    x = hid[...].astype(f32)
    inv_rms = lax.rsqrt(jnp.mean(x * x, axis=-1, keepdims=True) + EPSILON)
    xn[...] = (x * inv_rms * gain).astype(bf16)

    def project(w):
        y = jnp.dot(xn[...], w, preferred_element_type=f32)
        return y.astype(bf16)

    k_copy.wait()
    v_copy.wait()
    y = project(wkv[...]).astype(f32)
    kv[core, 0] = y[:, 0:half]
    kv[core, 1] = y[:, half:2 * half]
    pl.semaphore_wait(barrier, 1)
    kv_copy = pltpu.make_async_remote_copy(src_ref=kv.at[core], dst_ref=kv.at[core], send_sem=kv_s, recv_sem=kv_r,
                                           device_id=partner, device_id_type=MESH)
    kv_copy.start()

    def place(k, j, y):
        for i in range(q_ref.shape[1]):
            for d in range(2):
                q_ref[k, i, d, pl.ds(j, brows, stride=heads), :] = y[i * brows:(i + 1) * brows, d * half:(d + 1) * half]

    def one_head(j, carry):
        q_copy(j).wait()

        @pl.when(j + ahead < heads)
        def _():
            q_copy(j + ahead).start()

        y = project(wq[j]).astype(f32)
        mine[j] = (rotate(y, cos_t, sin_t) * head_dim ** -0.5).astype(bf16).astype(f32)
        exchange(j).start()
        place(core, j, mine[j])
        return carry

    lax.fori_loop(0, heads, one_head, 0)
    kv_copy.wait_recv()
    k_ref[...] = rotate(jnp.concatenate([kv[0, 0], kv[1, 0]], axis=-1), cos_t, sin_t).astype(bf16)
    v_ref[...] = jnp.concatenate([kv[0, 1], kv[1, 1]], axis=-1).astype(bf16)

    def their_head(j, carry):
        exchange(j).wait_recv()
        place(1 - core, j, theirs[j])
        return carry

    lax.fori_loop(0, heads, their_head, 0)
    kv_copy.wait_send()

    def finish(j, carry):
        exchange(j).wait_send()
        return carry

    lax.fori_loop(0, heads, finish, 0)


def attend_kernel(last_ref, q_all, kc_ref, vc_ref, hid_ref, wo_hbm, out_ref,
                  p_buf, mine, theirs, r_recv, l_recv, from_left, from_right, att, a_bf, wo, gath, other,
                  sem_wo, d_s, d_r, rs_s, rs_r, at_s, at_r, own_s, own_r, fw_s, fw_r, h_s, h_r):
    f32, bf16 = jnp.float32, jnp.bfloat16
    me = lax.axis_index('sp')
    chip, core = me // 2, lax.rem(me, 2)
    mate = 1 - core
    peers = 2 * CHIPS
    slots = kc_ref.shape[1]
    urows = 2 * CROWS
    hrows = CROWS // 2
    hl = att.shape[4]
    heads = att.shape[3] // CROWS
    hh = heads // 2
    hd = 2 * hl
    nq = wo.shape[0]
    nm = own_s.shape[2]
    per = nq // nm
    data = mine.shape[4] - 8

    def at(c, k):
        return {'sp': lax.rem(c + CHIPS, CHIPS) * 2 + k}

    right, left = at(chip + 1, core), at(chip - 1, core)
    partner = at(chip, mate)

    def remote(src, dst, ssem, rsem, dev):
        return pltpu.make_async_remote_copy(src_ref=src, dst_ref=dst, send_sem=ssem, recv_sem=rsem,
                                            device_id=dev, device_id_type=MESH)

    def wo_copy(j):
        columns = pl.ds(pl.multiple_of((core * nq + j) * hd, hd), hd)
        return pltpu.make_async_copy(wo_hbm.at[:, columns], wo.at[j], sem_wo.at[j])

    for j in range(nq):
        wo_copy(j).start()

    barrier = pltpu.get_barrier_semaphore()
    for dev in (right, left, partner):
        pl.semaphore_signal(barrier, inc=1, device_id=dev, device_id_type=MESH)

    lane = lax.broadcasted_iota(jnp.int32, (heads, slots), 1)
    lane8 = lax.broadcasted_iota(jnp.int32, (8, 128), 1)
    is_max = lane8 < 64

    def place_of(t):
        return lax.rem(chip + 2 - t + 3 * (t // 2) - 2 * (t // 3), CHIPS)

    def scores(ph, t):
        i = 2 * place_of(t) + ph
        for kk in range(2):
            for half in range(2):
                stat = jnp.zeros((8, 128), f32)
                for r4 in range(hrows):
                    r = kk * CROWS + half * hrows + r4
                    b = i * urows + r
                    own_rows = slice(r * hh, (r + 1) * hh)
                    q = jnp.concatenate([
                        jnp.concatenate([q_all[k, i, d, own_rows, :] for k in range(2)], axis=0) for d in range(2)], axis=1)
                    s = lax.dot_general(q.astype(bf16), kc_ref[b], (((1,), (1,)), ((), ())), preferred_element_type=f32)
                    valid = lane <= last_ref[pl.ds(b, 1), :]
                    s = jnp.where(valid, s, LOWEST)
                    m = jnp.max(s, axis=1, keepdims=True)
                    p = jnp.where(valid, jnp.exp(s - m), 0.0)
                    den = jnp.sum(p, axis=1, keepdims=True)
                    p_buf[t, r] = p.astype(bf16)
                    for g in range(2):
                        stat = jnp.where(lane8 == g * 32 + r4, m[g * 8:(g + 1) * 8],
                                         jnp.where(lane8 == 64 + g * 32 + r4, den[g * 8:(g + 1) * 8], stat))
                mine[ph, t, kk, half, data:data + 8, :] = stat

    def values(ph, t):
        i = 2 * place_of(t) + ph
        for kk in range(2):
            for half in range(2):
                for r4 in range(hrows):
                    r = kk * CROWS + half * hrows + r4
                    o = jnp.dot(p_buf[t, r], vc_ref[i * urows + r], preferred_element_type=f32)
                    for d in range(2):
                        rows = slice((d * hrows + r4) * heads, (d * hrows + r4 + 1) * heads)
                        mine[ph, t, kk, half, rows, :] = o[:, d * hl:(d + 1) * hl]

    def d_copy(ph, t):
        return remote(mine.at[ph, t, mate], theirs.at[ph, t], d_s.at[ph, t], d_r.at[ph, t], partner)

    def tiles():
        for r4 in range(hrows):
            for g in range(2):
                for d in range(2):
                    yield g * 32 + r4, (d * hrows + r4) * heads + g * 8, d, r4, g

    def merge(into, src):
        one, two = into[data:data + 8, :], src[data:data + 8, :]
        top = jnp.maximum(one, two)
        a, b = jnp.exp(one - top), jnp.exp(two - top)
        den = pltpu.roll(a, 64, 1) * one + pltpu.roll(b, 64, 1) * two
        for column, row, _, _, _ in tiles():
            into[row:row + 8, :] = (into[row:row + 8, :] * a[:, column:column + 1]
                                    + src[row:row + 8, :] * b[:, column:column + 1])
        into[data:data + 8, :] = jnp.where(is_max, top, den)

    def combine(ph, t):
        d_copy(ph, t).wait_recv()
        for half in range(2):
            merge(mine.at[ph, t, core, half], theirs.at[ph, t, half])

    def ring(ph, n, src, dst, dev):
        return remote(src, dst, rs_s.at[ph, n], rs_r.at[ph, n], dev)

    def piece(ph, t, half):
        return mine.at[ph, t, core, half]

    def r1(ph):
        return ring(ph, 0, piece(ph, 0, 0), r_recv.at[ph], right)

    def l1(ph):
        return ring(ph, 1, piece(ph, 0, 1), l_recv.at[ph], left)

    def r2(ph, half):
        return ring(ph, 2 + half, piece(ph, 1, half), from_left.at[ph, half], right)

    def l2(ph, half):
        return ring(ph, 4 + half, piece(ph, 2, half), from_right.at[ph, half], left)

    def reduce_far(ph):
        combine(ph, 0)
        r1(ph).start()
        l1(ph).start()

    def reduce_near(ph):
        combine(ph, 1)
        r2(ph, 1).start()
        combine(ph, 2)
        l2(ph, 0).start()

    def reduce_turn(ph):
        r1(ph).wait_recv()
        merge(piece(ph, 1, 0), r_recv.at[ph])
        r2(ph, 0).start()
        l1(ph).wait_recv()
        merge(piece(ph, 2, 1), l_recv.at[ph])
        l2(ph, 1).start()

    def at_copy(ph):
        return remote(att.at[ph, core], att.at[ph, core], at_s.at[ph], at_r.at[ph], partner)

    def reduce_end(ph):
        for half in range(2):
            r2(ph, half).wait_recv()
            l2(ph, half).wait_recv()
            parts = [mine.at[ph, 3, core, half], from_left.at[ph, half], from_right.at[ph, half]]
            stats = [x[data:data + 8, :] for x in parts]
            top = jnp.maximum(jnp.maximum(stats[0], stats[1]), stats[2])
            scale = [jnp.exp(x - top) for x in stats]
            den = sum(a * pltpu.roll(x, 64, 1) for a, x in zip(scale, stats))
            den = jnp.where(is_max & (lane8 % 32 < hrows), den, 1.0)
            scale = [a / den for a in scale]
            for column, row, d, r4, g in tiles():
                y = sum(x[row:row + 8, :] * a[:, column:column + 1] for x, a in zip(parts, scale))
                to = (half * hrows + r4) * heads + g * 8
                att[ph, core, d, to:to + 8, :] = y
        at_copy(ph).start()

    def rows_of(c, ph):
        return pl.ds(pl.multiple_of((2 * c + ph) * urows, urows), urows)

    def columns_of(k, n):
        return pl.ds(pl.multiple_of((k * nq + n) * hd, hd), hd)

    def own_copies(ph, u):
        src = gath.at[ph, chip, pl.ds(u * per, per)]
        return (remote(src, src, own_s.at[ph, 0, u], own_r.at[ph, 0, u], right),
                remote(src, src, own_s.at[ph, 1, u], own_r.at[ph, 1, u], left),
                to_mate(ph, 0, chip, u))

    def to_mate(ph, which, c, u):
        part = pl.ds(u * per, per)
        return remote(gath.at[ph, c, part], other.at[ph, c, part], h_s.at[ph, which, u], h_r.at[ph, which, u], partner)

    def gather_rows(ph):
        at_copy(ph).wait_recv()
        for h in range(heads):
            for d in range(2):
                pair = [att[ph, kk, d, pl.ds(h, CROWS, stride=heads), :] for kk in range(2)]
                a_bf[ph, :, h * hd + d * hl:h * hd + (d + 1) * hl] = jnp.concatenate(pair, axis=0).astype(bf16)

    def project(ph, u):
        for n in range(u * per, (u + 1) * per):
            if ph == 0:
                wo_copy(n).wait()
            y = jnp.dot(a_bf[ph], wo[n], preferred_element_type=f32)
            gath[ph, chip, n] = hid_ref[rows_of(chip, ph), columns_of(core, n)].astype(f32) + y
        for copy in own_copies(ph, u):
            copy.start()

    cl, cr, co = place_of(2), place_of(1), place_of(0)
    split = nm // 2

    def forward(ph, way, u):
        c, dev = (cl, right) if way == 0 else (cr, left)
        src = gath.at[ph, c, pl.ds(u * per + way * (per // 2), per // 2)]
        return remote(src, src, fw_s.at[ph, way, u], fw_r.at[ph, way, u], dev)

    def put(ph, c, u):
        for n in range(u * per, (u + 1) * per):
            out_ref[rows_of(c, ph), columns_of(core, n)] = gath[ph, c, n].astype(bf16)

    def put_other(ph, c, u):
        for n in range(u * per, (u + 1) * per):
            out_ref[rows_of(c, ph), columns_of(mate, n)] = other[ph, c, n].astype(bf16)

    def relay(ph, u):
        own_copies(ph, u)[0].wait_recv()
        forward(ph, 0, u).start()
        to_mate(ph, 1, cl, u).start()
        own_copies(ph, u)[1].wait_recv()
        forward(ph, 1, u).start()
        to_mate(ph, 2, cr, u).start()

    def relay_end(ph):
        for u in range(nm):
            for way in range(2):
                forward(ph, way, u).wait_recv()
            to_mate(ph, 3, co, u).start()

    places = ((0, chip), (1, cl), (2, cr), (3, co))

    def finish(ph):
        for which, c in places:
            for u in range(nm):
                put(ph, c, u)
                to_mate(ph, which, c, u).wait_recv()
                put_other(ph, c, u)

    def units(ph, first, last, send):
        def body(t, carry):
            scores(ph, t)
            values(ph, t)
            if send:
                d_copy(ph, t).start()
            return carry

        lax.fori_loop(first, last, body, 0)

    units(0, 0, 2, False)
    pl.semaphore_wait(barrier, 3)
    d_copy(0, 0).start()
    d_copy(0, 1).start()
    units(0, 2, CHIPS, True)
    reduce_far(0)
    reduce_near(0)
    units(1, 0, CHIPS, True)
    reduce_far(1)
    reduce_turn(0)
    reduce_near(1)
    combine(0, 3)
    reduce_turn(1)
    combine(1, 3)
    reduce_end(0)
    gather_rows(0)
    for u in range(split):
        project(0, u)
    reduce_end(1)
    for u in range(split, nm):
        project(0, u)
    for u in range(split):
        relay(0, u)
    gather_rows(1)
    for u in range(nm):
        project(1, u)
        if u < nm - split:
            relay(0, split + u)
    for u in range(split):
        relay(1, u)
    relay_end(0)
    for u in range(split, nm):
        relay(1, u)
    finish(0)
    relay_end(1)
    finish(1)

    for ph in range(2):
        for t in range(CHIPS):
            d_copy(ph, t).wait_send()
        for copy in (r1(ph), l1(ph), r2(ph, 0), r2(ph, 1), l2(ph, 0), l2(ph, 1), at_copy(ph)):
            copy.wait_send()
        for u in range(nm):
            for copy in own_copies(ph, u):
                copy.wait_send()
            for way in range(2):
                forward(ph, way, u).wait_send()
            for which, c in places[1:]:
                to_mate(ph, which, c, u).wait_send()


def local_step(hidden, w_norm, w_q, w_k, w_v, w_o, k_block, v_block, cache_len):
    f32, bf16 = jnp.float32, jnp.bfloat16
    rows, width = hidden.shape
    seq_block, hd = k_block.shape[1], k_block.shape[2]
    heads = w_q.shape[1] // hd
    hh, hl = heads // 2, hd // 2
    nblk = 2 * CHIPS
    brows = rows // nblk
    assert brows == 2 * CROWS
    inv_freq = (ROPE_BASE ** (-jnp.arange(hl, dtype=f32) * 2.0 / hd)).reshape(1, hl)
    vmem = pl.BlockSpec(memory_space=pltpu.VMEM)
    hbm = pl.BlockSpec(memory_space=pl.ANY)
    dma = pltpu.SemaphoreType.DMA

    def keep(x):
        return pltpu.with_memory_space_constraint(x, pltpu.HBM)

    def near(x):
        return pltpu.with_memory_space_constraint(x, pltpu.VMEM)

    q_all, k_rot, v_new, slot, last = pl.pallas_call(
        functools.partial(project_kernel, seq_block),
        out_shape=(pltpu.VMEM((2, nblk, 2, brows * hh, hl), f32), jax.ShapeDtypeStruct((rows, hd), bf16),
                   jax.ShapeDtypeStruct((rows, hd), bf16), jax.ShapeDtypeStruct((rows, seq_block), jnp.int32),
                   jax.ShapeDtypeStruct((rows, seq_block), jnp.int32)),
        in_specs=[hbm] * 3 + [vmem] + [hbm] * 3,
        out_specs=(vmem,) * 5,
        scratch_shapes=[
            pltpu.VMEM((rows,), jnp.int32),
            pltpu.VMEM((width,), bf16),
            pltpu.VMEM((rows, width), bf16),
            pltpu.VMEM((rows, width), bf16),
            pltpu.VMEM((width, hd), bf16),
            pltpu.VMEM((hh, width, hd), bf16),
            pltpu.VMEM((2, 2, rows, hl), f32),
            pltpu.VMEM((hh, rows, hd), f32),
            pltpu.VMEM((hh, rows, hd), f32),
            dma, dma, dma, dma, dma, dma((hh,)), dma, dma, dma((hh,)), dma((hh,)),
        ],
        compiler_params=pltpu.CompilerParams(collective_id=1, has_side_effects=True, vmem_limit_bytes=48 * MIB),
        cost_estimate=pl.CostEstimate(flops=2 * rows * width * (hh + 1) * hd, bytes_accessed=2 * width * (hh + 1) * hd,
                                      transcendentals=0),
        name='project',
    )(keep(cache_len), keep(hidden), keep(w_norm), inv_freq, keep(w_k), keep(w_v), keep(w_q))

    at_slot = (slot != 0)[:, :, None]
    new_k_block = jnp.where(at_slot, k_rot[:, None, :], k_block)
    new_v_block = jnp.where(at_slot, v_new[:, None, :], v_block)

    half_rows = CROWS * heads + 8
    nm = hh // 2
    out_hidden = pl.pallas_call(
        attend_kernel,
        out_shape=jax.ShapeDtypeStruct((rows, width), bf16),
        in_specs=[vmem, vmem, vmem, vmem, vmem, hbm],
        out_specs=vmem,
        scratch_shapes=[
            pltpu.VMEM((CHIPS, brows, heads, seq_block), bf16),
            pltpu.VMEM((2, CHIPS, 2, 2, half_rows, hl), f32),
            pltpu.VMEM((2, CHIPS, 2, half_rows, hl), f32),
            pltpu.VMEM((2, half_rows, hl), f32),
            pltpu.VMEM((2, half_rows, hl), f32),
            pltpu.VMEM((2, 2, half_rows, hl), f32),
            pltpu.VMEM((2, 2, half_rows, hl), f32),
            pltpu.VMEM((2, 2, 2, CROWS * heads, hl), f32),
            pltpu.VMEM((2, brows, width), bf16),
            pltpu.VMEM((hh, width, hd), bf16),
            pltpu.VMEM((2, CHIPS, hh, brows, hd), f32),
            pltpu.VMEM((2, CHIPS, hh, brows, hd), f32),
            dma((hh,)), dma((2, CHIPS)), dma((2, CHIPS)), dma((2, 6)), dma((2, 6)), dma((2,)), dma((2,)),
            dma((2, 2, nm)), dma((2, 2, nm)), dma((2, 2, nm)), dma((2, 2, nm)), dma((2, CHIPS, nm)), dma((2, CHIPS, nm)),
        ],
        compiler_params=pltpu.CompilerParams(collective_id=0, has_side_effects=True, vmem_limit_bytes=26 * MIB),
        cost_estimate=pl.CostEstimate(flops=2 * rows * width * hh * hd * 2, bytes_accessed=2 * width * hh * hd,
                                      transcendentals=0),
        name='attend',
    )(last, near(q_all), near(new_k_block), near(new_v_block), hidden, keep(w_o))
    return out_hidden, new_k_block, new_v_block


def solution(mesh):
    assert mesh.shape['sp'] == 2 * CHIPS
    cache_spec = P('dp', 'sp', None)
    return jax.shard_map(local_step, mesh=mesh, in_specs=(P('dp', None), P(None), P(None, None), P(None, None), P(None, None), P(None, None), cache_spec, cache_spec, P('dp')), out_specs=(P('dp', None), cache_spec, cache_spec), check_vma=False)
```

```python
import functools

import jax
import jax.numpy as jnp
from jax import lax
from jax.experimental import pallas as pl
from jax.experimental.pallas import tpu as pltpu
from jax.sharding import PartitionSpec as P

ROPE_BASE = 10000.0
EPSILON = 1e-6
MESH = pl.DeviceIdType.MESH
MIB = 1 << 20
LOWEST = float(jnp.finfo(jnp.float32).min)
CROWS = 8
CHIPS = 4


def rotate(x, cos_t, sin_t):
    half = x.shape[-1] // 2
    low, high = x[:, :half], x[:, half:]
    return jnp.concatenate([low * cos_t - high * sin_t, high * cos_t + low * sin_t], axis=-1)


def project_kernel(slots, len_hbm, hid_hbm, wn_hbm, fr_ref, wk_hbm, wv_hbm, wq_hbm, q_ref, k_ref, v_ref, slot_ref, last_ref,
                   lens, wn, hid, xn, wkv, wq, kv, mine, theirs, sem_l, sem_n, sem_h, sem_k, sem_v, sem_q, kv_s, kv_r,
                   x_s, x_r):
    f32, bf16 = jnp.float32, jnp.bfloat16
    rows = hid.shape[0]
    head_dim = wq.shape[2]
    heads, half = wq.shape[0], head_dim // 2
    brows = rows // q_ref.shape[1]
    me = lax.axis_index('sp')
    core = lax.rem(me, 2)
    partner = {'sp': me + 1 - 2 * core}

    def q_copy(j):
        columns = pl.ds(pl.multiple_of((core * heads + j) * head_dim, head_dim), head_dim)
        return pltpu.make_async_copy(wq_hbm.at[:, columns], wq.at[j], sem_q.at[j])

    def exchange(j):
        return pltpu.make_async_remote_copy(src_ref=mine.at[j], dst_ref=theirs.at[j], send_sem=x_s.at[j],
                                            recv_sem=x_r.at[j], device_id=partner, device_id_type=MESH)

    part = pl.ds(pl.multiple_of(core * half, half), half)
    l_copy = pltpu.make_async_copy(len_hbm, lens, sem_l)
    n_copy = pltpu.make_async_copy(wn_hbm, wn, sem_n)
    h_copy = pltpu.make_async_copy(hid_hbm, hid, sem_h)
    k_copy = pltpu.make_async_copy(wk_hbm.at[:, part], wkv.at[:, pl.ds(0, half)], sem_k)
    v_copy = pltpu.make_async_copy(wv_hbm.at[:, part], wkv.at[:, pl.ds(half, half)], sem_v)
    for copy in (h_copy, l_copy, n_copy, k_copy, v_copy):
        copy.start()
    ahead = 5
    for j in range(2):
        q_copy(j).start()
    barrier = pltpu.get_barrier_semaphore()
    pl.semaphore_signal(barrier, inc=1, device_id=partner, device_id_type=MESH)

    l_copy.wait()
    lengths = lens[...].reshape(1, rows)
    across = lax.broadcasted_iota(jnp.int32, (rows, rows), 1)
    down = lax.broadcasted_iota(jnp.int32, (rows, rows), 0)
    column = jnp.sum(jnp.where(across == down, lengths, 0).astype(f32), axis=1, keepdims=True)
    slot = lax.broadcasted_iota(jnp.int32, (rows, slots), 1) + me * slots
    slot_ref[...] = (slot.astype(f32) == column).astype(jnp.int32)
    last_ref[...] = jnp.broadcast_to(column.astype(jnp.int32) - me * slots, last_ref.shape)
    angles = column * fr_ref[...]
    cos_t, sin_t = jnp.cos(angles), jnp.sin(angles)

    n_copy.wait()
    gain = 1.0 + wn[...].astype(f32).reshape(1, wn.shape[0])
    h_copy.wait()
    for j in range(2, ahead):
        q_copy(j).start()
    x = hid[...].astype(f32)
    inv_rms = lax.rsqrt(jnp.mean(x * x, axis=-1, keepdims=True) + EPSILON)
    xn[...] = (x * inv_rms * gain).astype(bf16)

    def project(w):
        y = jnp.dot(xn[...], w, preferred_element_type=f32)
        return y.astype(bf16)

    k_copy.wait()
    v_copy.wait()
    y = project(wkv[...]).astype(f32)
    kv[core, 0] = y[:, 0:half]
    kv[core, 1] = y[:, half:2 * half]
    pl.semaphore_wait(barrier, 1)
    kv_copy = pltpu.make_async_remote_copy(src_ref=kv.at[core], dst_ref=kv.at[core], send_sem=kv_s, recv_sem=kv_r,
                                           device_id=partner, device_id_type=MESH)
    kv_copy.start()

    def place(k, j, y):
        for i in range(q_ref.shape[1]):
            for d in range(2):
                q_ref[k, i, d, pl.ds(j, brows, stride=heads), :] = y[i * brows:(i + 1) * brows, d * half:(d + 1) * half]

    def one_head(j, carry):
        q_copy(j).wait()

        @pl.when(j + ahead < heads)
        def _():
            q_copy(j + ahead).start()

        y = project(wq[j]).astype(f32)
        mine[j] = (rotate(y, cos_t, sin_t) * head_dim ** -0.5).astype(bf16).astype(f32)
        exchange(j).start()
        place(core, j, mine[j])
        return carry

    lax.fori_loop(0, heads, one_head, 0)
    kv_copy.wait_recv()
    k_ref[...] = rotate(jnp.concatenate([kv[0, 0], kv[1, 0]], axis=-1), cos_t, sin_t).astype(bf16)
    v_ref[...] = jnp.concatenate([kv[0, 1], kv[1, 1]], axis=-1).astype(bf16)

    def their_head(j, carry):
        exchange(j).wait_recv()
        place(1 - core, j, theirs[j])
        return carry

    lax.fori_loop(0, heads, their_head, 0)
    kv_copy.wait_send()

    def finish(j, carry):
        exchange(j).wait_send()
        return carry

    lax.fori_loop(0, heads, finish, 0)


def attend_kernel(last_ref, q_all, kc_ref, vc_ref, hid_ref, wo_hbm, out_ref,
                  p_buf, mine, theirs, r_recv, l_recv, from_left, from_right, att, a_bf, wo, gath, other,
                  sem_wo, d_s, d_r, rs_s, rs_r, at_s, at_r, own_s, own_r, fw_s, fw_r, h_s, h_r):
    f32, bf16 = jnp.float32, jnp.bfloat16
    me = lax.axis_index('sp')
    chip, core = me // 2, lax.rem(me, 2)
    mate = 1 - core
    peers = 2 * CHIPS
    slots = kc_ref.shape[1]
    urows = 2 * CROWS
    hrows = CROWS // 2
    hl = att.shape[4]
    heads = att.shape[3] // CROWS
    hh = heads // 2
    hd = 2 * hl
    nq = wo.shape[0]
    nm = own_s.shape[2]
    per = nq // nm
    data = mine.shape[4] - 8

    def at(c, k):
        return {'sp': lax.rem(c + CHIPS, CHIPS) * 2 + k}

    right, left = at(chip + 1, core), at(chip - 1, core)
    partner = at(chip, mate)

    def remote(src, dst, ssem, rsem, dev):
        return pltpu.make_async_remote_copy(src_ref=src, dst_ref=dst, send_sem=ssem, recv_sem=rsem,
                                            device_id=dev, device_id_type=MESH)

    def wo_copy(j):
        columns = pl.ds(pl.multiple_of((core * nq + j) * hd, hd), hd)
        return pltpu.make_async_copy(wo_hbm.at[:, columns], wo.at[j], sem_wo.at[j])

    for j in range(nq):
        wo_copy(j).start()

    barrier = pltpu.get_barrier_semaphore()
    for dev in (right, left, partner):
        pl.semaphore_signal(barrier, inc=1, device_id=dev, device_id_type=MESH)

    lane = lax.broadcasted_iota(jnp.int32, (heads, slots), 1)
    lane8 = lax.broadcasted_iota(jnp.int32, (8, 128), 1)
    is_max = lane8 < 64

    def place_of(t):
        return lax.rem(chip + 2 - t + 3 * (t // 2) - 2 * (t // 3), CHIPS)

    def scores(ph, t):
        i = 2 * place_of(t) + ph
        for kk in range(2):
            for half in range(2):
                stat = jnp.zeros((8, 128), f32)
                for r4 in range(hrows):
                    r = kk * CROWS + half * hrows + r4
                    b = i * urows + r
                    own_rows = slice(r * hh, (r + 1) * hh)
                    q = jnp.concatenate([
                        jnp.concatenate([q_all[k, i, d, own_rows, :] for k in range(2)], axis=0) for d in range(2)], axis=1)
                    s = lax.dot_general(q.astype(bf16), kc_ref[b], (((1,), (1,)), ((), ())), preferred_element_type=f32)
                    valid = lane <= last_ref[pl.ds(b, 1), :]
                    s = jnp.where(valid, s, LOWEST)
                    m = jnp.max(s, axis=1, keepdims=True)
                    p = jnp.where(valid, jnp.exp(s - m), 0.0)
                    den = jnp.sum(p, axis=1, keepdims=True)
                    p_buf[t, r] = p.astype(bf16)
                    for g in range(2):
                        stat = jnp.where(lane8 == g * 32 + r4, m[g * 8:(g + 1) * 8],
                                         jnp.where(lane8 == 64 + g * 32 + r4, den[g * 8:(g + 1) * 8], stat))
                mine[ph, t, kk, half, data:data + 8, :] = stat

    def values(ph, t):
        i = 2 * place_of(t) + ph
        for kk in range(2):
            for half in range(2):
                for r4 in range(hrows):
                    r = kk * CROWS + half * hrows + r4
                    o = jnp.dot(p_buf[t, r], vc_ref[i * urows + r], preferred_element_type=f32)
                    for d in range(2):
                        rows = slice((d * hrows + r4) * heads, (d * hrows + r4 + 1) * heads)
                        mine[ph, t, kk, half, rows, :] = o[:, d * hl:(d + 1) * hl]

    def d_copy(ph, t):
        return remote(mine.at[ph, t, mate], theirs.at[ph, t], d_s.at[ph, t], d_r.at[ph, t], partner)

    def tiles():
        for r4 in range(hrows):
            for g in range(2):
                for d in range(2):
                    yield g * 32 + r4, (d * hrows + r4) * heads + g * 8, d, r4, g

    def merge(into, src):
        one, two = into[data:data + 8, :], src[data:data + 8, :]
        top = jnp.maximum(one, two)
        a, b = jnp.exp(one - top), jnp.exp(two - top)
        den = pltpu.roll(a, 64, 1) * one + pltpu.roll(b, 64, 1) * two
        for column, row, _, _, _ in tiles():
            into[row:row + 8, :] = (into[row:row + 8, :] * a[:, column:column + 1]
                                    + src[row:row + 8, :] * b[:, column:column + 1])
        into[data:data + 8, :] = jnp.where(is_max, top, den)

    def combine(ph, t):
        d_copy(ph, t).wait_recv()
        for half in range(2):
            merge(mine.at[ph, t, core, half], theirs.at[ph, t, half])

    def ring(ph, n, src, dst, dev):
        return remote(src, dst, rs_s.at[ph, n], rs_r.at[ph, n], dev)

    def piece(ph, t, half):
        return mine.at[ph, t, core, half]

    def r1(ph):
        return ring(ph, 0, piece(ph, 0, 0), r_recv.at[ph], right)

    def l1(ph):
        return ring(ph, 1, piece(ph, 0, 1), l_recv.at[ph], left)

    def r2(ph, half):
        return ring(ph, 2 + half, piece(ph, 1, half), from_left.at[ph, half], right)

    def l2(ph, half):
        return ring(ph, 4 + half, piece(ph, 2, half), from_right.at[ph, half], left)

    def reduce_far(ph):
        combine(ph, 0)
        r1(ph).start()
        l1(ph).start()

    def reduce_near(ph):
        combine(ph, 1)
        r2(ph, 1).start()
        combine(ph, 2)
        l2(ph, 0).start()

    def reduce_turn(ph):
        r1(ph).wait_recv()
        merge(piece(ph, 1, 0), r_recv.at[ph])
        r2(ph, 0).start()
        l1(ph).wait_recv()
        merge(piece(ph, 2, 1), l_recv.at[ph])
        l2(ph, 1).start()

    def at_copy(ph):
        return remote(att.at[ph, core], att.at[ph, core], at_s.at[ph], at_r.at[ph], partner)

    def reduce_end(ph):
        for half in range(2):
            r2(ph, half).wait_recv()
            l2(ph, half).wait_recv()
            parts = [mine.at[ph, 3, core, half], from_left.at[ph, half], from_right.at[ph, half]]
            stats = [x[data:data + 8, :] for x in parts]
            top = jnp.maximum(jnp.maximum(stats[0], stats[1]), stats[2])
            scale = [jnp.exp(x - top) for x in stats]
            den = sum(a * pltpu.roll(x, 64, 1) for a, x in zip(scale, stats))
            den = jnp.where(is_max & (lane8 % 32 < hrows), den, 1.0)
            scale = [a / den for a in scale]
            for column, row, d, r4, g in tiles():
                y = sum(x[row:row + 8, :] * a[:, column:column + 1] for x, a in zip(parts, scale))
                to = (half * hrows + r4) * heads + g * 8
                att[ph, core, d, to:to + 8, :] = y
        at_copy(ph).start()

    def rows_of(c, ph):
        return pl.ds(pl.multiple_of((2 * c + ph) * urows, urows), urows)

    def columns_of(k, n):
        return pl.ds(pl.multiple_of((k * nq + n) * hd, hd), hd)

    def own_copies(ph, u):
        src = gath.at[ph, chip, pl.ds(u * per, per)]
        return (remote(src, src, own_s.at[ph, 0, u], own_r.at[ph, 0, u], right),
                remote(src, src, own_s.at[ph, 1, u], own_r.at[ph, 1, u], left),
                to_mate(ph, 0, chip, u))

    def to_mate(ph, which, c, u):
        part = pl.ds(u * per, per)
        return remote(gath.at[ph, c, part], other.at[ph, c, part], h_s.at[ph, which, u], h_r.at[ph, which, u], partner)

    def gather_rows(ph):
        at_copy(ph).wait_recv()
        for h in range(heads):
            for d in range(2):
                pair = [att[ph, kk, d, pl.ds(h, CROWS, stride=heads), :] for kk in range(2)]
                a_bf[ph, :, h * hd + d * hl:h * hd + (d + 1) * hl] = jnp.concatenate(pair, axis=0).astype(bf16)

    def project(ph, u):
        for n in range(u * per, (u + 1) * per):
            if ph == 0:
                wo_copy(n).wait()
            y = jnp.dot(a_bf[ph], wo[n], preferred_element_type=f32)
            gath[ph, chip, n] = hid_ref[rows_of(chip, ph), columns_of(core, n)].astype(f32) + y
        for copy in own_copies(ph, u):
            copy.start()

    cl, cr, co = place_of(2), place_of(1), place_of(0)
    split = nm // 2

    def forward(ph, way, u):
        c, dev = (cl, right) if way == 0 else (cr, left)
        src = gath.at[ph, c, pl.ds(u * per + way * (per // 2), per // 2)]
        return remote(src, src, fw_s.at[ph, way, u], fw_r.at[ph, way, u], dev)

    def put(ph, c, u):
        for n in range(u * per, (u + 1) * per):
            out_ref[rows_of(c, ph), columns_of(core, n)] = gath[ph, c, n].astype(bf16)

    def put_other(ph, c, u):
        for n in range(u * per, (u + 1) * per):
            out_ref[rows_of(c, ph), columns_of(mate, n)] = other[ph, c, n].astype(bf16)

    def relay(ph, u):
        own_copies(ph, u)[0].wait_recv()
        forward(ph, 0, u).start()
        to_mate(ph, 1, cl, u).start()
        own_copies(ph, u)[1].wait_recv()
        forward(ph, 1, u).start()
        to_mate(ph, 2, cr, u).start()

    def relay_end(ph):
        for u in range(nm):
            for way in range(2):
                forward(ph, way, u).wait_recv()
            to_mate(ph, 3, co, u).start()
            put(ph, co, u)

    places = ((0, chip), (1, cl), (2, cr), (3, co))

    def finish(ph, which):
        c = places[which][1]
        for u in range(nm):
            if which < 3:
                put(ph, c, u)
            to_mate(ph, which, c, u).wait_recv()
            put_other(ph, c, u)

    def units(ph, first, last, send):
        def body(t, carry):
            scores(ph, t)
            values(ph, t)
            if send:
                d_copy(ph, t).start()
            return carry

        lax.fori_loop(first, last, body, 0)

    units(0, 0, 2, False)
    pl.semaphore_wait(barrier, 3)
    d_copy(0, 0).start()
    d_copy(0, 1).start()
    units(0, 2, CHIPS, True)
    reduce_far(0)
    reduce_near(0)
    units(1, 0, CHIPS, True)
    reduce_far(1)
    combine(0, 3)
    reduce_turn(0)
    reduce_near(1)
    reduce_turn(1)
    combine(1, 3)
    reduce_end(0)
    gather_rows(0)
    for u in range(split):
        project(0, u)
    reduce_end(1)
    for u in range(split, nm):
        project(0, u)
    for u in range(split):
        relay(0, u)
    gather_rows(1)
    for u in range(nm):
        project(1, u)
        if u < nm - split:
            relay(0, split + u)
    for u in range(split):
        relay(1, u)
    relay_end(0)
    for u in range(split, nm):
        relay(1, u)
    for which in range(4):
        finish(0, which)
    for which in range(3):
        finish(1, which)
    relay_end(1)
    finish(1, 3)

    for ph in range(2):
        for t in range(CHIPS):
            d_copy(ph, t).wait_send()
        for copy in (r1(ph), l1(ph), r2(ph, 0), r2(ph, 1), l2(ph, 0), l2(ph, 1), at_copy(ph)):
            copy.wait_send()
        for u in range(nm):
            for copy in own_copies(ph, u):
                copy.wait_send()
            for way in range(2):
                forward(ph, way, u).wait_send()
            for which, c in places[1:]:
                to_mate(ph, which, c, u).wait_send()


def local_step(hidden, w_norm, w_q, w_k, w_v, w_o, k_block, v_block, cache_len):
    f32, bf16 = jnp.float32, jnp.bfloat16
    rows, width = hidden.shape
    seq_block, hd = k_block.shape[1], k_block.shape[2]
    heads = w_q.shape[1] // hd
    hh, hl = heads // 2, hd // 2
    nblk = 2 * CHIPS
    brows = rows // nblk
    assert brows == 2 * CROWS
    inv_freq = (ROPE_BASE ** (-jnp.arange(hl, dtype=f32) * 2.0 / hd)).reshape(1, hl)
    vmem = pl.BlockSpec(memory_space=pltpu.VMEM)
    hbm = pl.BlockSpec(memory_space=pl.ANY)
    dma = pltpu.SemaphoreType.DMA

    def keep(x):
        return pltpu.with_memory_space_constraint(x, pltpu.HBM)

    def near(x):
        return pltpu.with_memory_space_constraint(x, pltpu.VMEM)

    q_all, k_rot, v_new, slot, last = pl.pallas_call(
        functools.partial(project_kernel, seq_block),
        out_shape=(pltpu.VMEM((2, nblk, 2, brows * hh, hl), f32), jax.ShapeDtypeStruct((rows, hd), bf16),
                   jax.ShapeDtypeStruct((rows, hd), bf16), jax.ShapeDtypeStruct((rows, seq_block), jnp.int32),
                   jax.ShapeDtypeStruct((rows, seq_block), jnp.int32)),
        in_specs=[hbm] * 3 + [vmem] + [hbm] * 3,
        out_specs=(vmem,) * 5,
        scratch_shapes=[
            pltpu.VMEM((rows,), jnp.int32),
            pltpu.VMEM((width,), bf16),
            pltpu.VMEM((rows, width), bf16),
            pltpu.VMEM((rows, width), bf16),
            pltpu.VMEM((width, hd), bf16),
            pltpu.VMEM((hh, width, hd), bf16),
            pltpu.VMEM((2, 2, rows, hl), f32),
            pltpu.VMEM((hh, rows, hd), f32),
            pltpu.VMEM((hh, rows, hd), f32),
            dma, dma, dma, dma, dma, dma((hh,)), dma, dma, dma((hh,)), dma((hh,)),
        ],
        compiler_params=pltpu.CompilerParams(collective_id=1, has_side_effects=True, vmem_limit_bytes=48 * MIB),
        cost_estimate=pl.CostEstimate(flops=2 * rows * width * (hh + 1) * hd, bytes_accessed=2 * width * (hh + 1) * hd,
                                      transcendentals=0),
        name='project',
    )(keep(cache_len), keep(hidden), keep(w_norm), inv_freq, keep(w_k), keep(w_v), keep(w_q))

    at_slot = (slot != 0)[:, :, None]
    new_k_block = jnp.where(at_slot, k_rot[:, None, :], k_block)
    new_v_block = jnp.where(at_slot, v_new[:, None, :], v_block)

    half_rows = CROWS * heads + 8
    nm = hh // 2
    out_hidden = pl.pallas_call(
        attend_kernel,
        out_shape=jax.ShapeDtypeStruct((rows, width), bf16),
        in_specs=[vmem, vmem, vmem, vmem, vmem, hbm],
        out_specs=vmem,
        scratch_shapes=[
            pltpu.VMEM((CHIPS, brows, heads, seq_block), bf16),
            pltpu.VMEM((2, CHIPS, 2, 2, half_rows, hl), f32),
            pltpu.VMEM((2, CHIPS, 2, half_rows, hl), f32),
            pltpu.VMEM((2, half_rows, hl), f32),
            pltpu.VMEM((2, half_rows, hl), f32),
            pltpu.VMEM((2, 2, half_rows, hl), f32),
            pltpu.VMEM((2, 2, half_rows, hl), f32),
            pltpu.VMEM((2, 2, 2, CROWS * heads, hl), f32),
            pltpu.VMEM((2, brows, width), bf16),
            pltpu.VMEM((hh, width, hd), bf16),
            pltpu.VMEM((2, CHIPS, hh, brows, hd), f32),
            pltpu.VMEM((2, CHIPS, hh, brows, hd), f32),
            dma((hh,)), dma((2, CHIPS)), dma((2, CHIPS)), dma((2, 6)), dma((2, 6)), dma((2,)), dma((2,)),
            dma((2, 2, nm)), dma((2, 2, nm)), dma((2, 2, nm)), dma((2, 2, nm)), dma((2, CHIPS, nm)), dma((2, CHIPS, nm)),
        ],
        compiler_params=pltpu.CompilerParams(collective_id=0, has_side_effects=True, vmem_limit_bytes=26 * MIB),
        cost_estimate=pl.CostEstimate(flops=2 * rows * width * hh * hd * 2, bytes_accessed=2 * width * hh * hd,
                                      transcendentals=0),
        name='attend',
    )(last, near(q_all), near(new_k_block), near(new_v_block), hidden, keep(w_o))
    return out_hidden, new_k_block, new_v_block


def solution(mesh):
    assert mesh.shape['sp'] == 2 * CHIPS
    cache_spec = P('dp', 'sp', None)
    return jax.shard_map(local_step, mesh=mesh, in_specs=(P('dp', None), P(None), P(None, None), P(None, None), P(None, None), P(None, None), cache_spec, cache_spec, P('dp')), out_specs=(P('dp', None), cache_spec, cache_spec), check_vma=False)
```
